32 devices in a mesh: ea: 8 (over z, y), ba: 4 (over x, core).
Axes of the slice: x: 2, y: 2, z: 4, core: 2. Of those that a mesh axis runs over, the one named last changes fastest.
Arguments:
- entities: float32 [4096, 200], P('ea'), may hold values from -1.5 to 1.5
- entity_history: float32 [4096], P('ea'), may hold values from 0.001 to 0.1
- relations: float32 [256, 200], replicated, may hold values from -6 to 6
- relation_history: float32 [256], replicated, may hold values from 0.001 to 0.1
- edge_ends: int32 [8192, 2], P(('ba', 'ea')), may hold values from 0 to 4095, as said below
- edge_relations: int32 [8192], P(('ba', 'ea')), may hold values from 0 to 255
- negatives: int32 [8192], P(('ba', 'ea')), may hold values from 0 to 4095, as said below
Outputs:
- entity_step: float32 [4096, 200], P('ea')
- entity_squares: float32 [4096], P('ea')
- relation_step: float32 [256, 200], replicated
- relation_squares: float32 [256], replicated
- mean_loss: float32 [1], replicated
The draws below stay inside these ranges and needn't reach their ends.
Inputs may be any that keep to these rules, and one draw needn't show every extreme that they name: `edge_ends`: every entry is an entity id. In each aligned block of 256 edges at most 48 heads have the same owner shard (id // 512), and some shard has exactly 48; the same holds for the tails. Every entry is an entity id. In each run of 256 consecutive negatives at most 48 have the same owner shard (id // 512), and some shard has exactly 48. `edge_relations`: every entry is a relation id.
All inputs are finite; a program needn't handle non-finite values.
Results may differ from the reference program's by a relative error of at most 0.0003.
Values sent between devices are 32-bit elements.
A program may use at most 64 MiB of HBM per device.

```python
import math
import jax
import jax.numpy as jnp
import numpy as np
from jax import lax

DIM = 200
RELS = 256
ENT_DEV = 512
EDGE_DEV = 256
NEG_DEV = 256
ENTITIES = 4096
EDGES = 8192
N_EA = 8
N_BA = 4


def relabels(key):
    blocks = N_BA * N_EA
    keys = jax.random.split(jax.random.fold_in(key, 11), blocks)
    return jax.vmap(lambda single: jax.random.permutation(single, N_EA))(keys).astype(jnp.int32)


def owned_ids(key, relabel, per_block):
    blocks = N_BA * N_EA
    mean_count = per_block // N_EA
    spread = max(1, mean_count // 2)
    lift_key, shuffle_key, row_key = jax.random.split(key, 3)
    lifted = jax.random.randint(lift_key, (blocks, N_EA // 2), 0, spread + 1).astype(jnp.int32)
    lifted = lifted.at[:, 0].set(spread)
    counts = jnp.stack([mean_count + lifted, mean_count - lifted], axis=2).reshape(blocks, N_EA)
    bounds = jnp.cumsum(counts, axis=1).astype(jnp.int32)
    slot_positions = jnp.arange(per_block, dtype=jnp.int32)
    sorted_owner = jax.vmap(lambda bound_row: jnp.searchsorted(bound_row, slot_positions, side='right'))(bounds)
    sorted_owner = sorted_owner.astype(jnp.int32)
    shuffle_keys = jax.random.split(shuffle_key, blocks)
    shuffle_order = jax.vmap(lambda single: jax.random.permutation(single, per_block))(shuffle_keys)
    shuffled = jnp.take_along_axis(sorted_owner, shuffle_order.astype(jnp.int32), axis=1)
    owners = jnp.take_along_axis(relabel, shuffled, axis=1)
    row_ids = jax.random.randint(row_key, (blocks, per_block), 0, ENT_DEV).astype(jnp.int32)
    return (owners * ENT_DEV + row_ids).reshape(-1).astype(jnp.int32)


def draw_edge_ends(key, part):
    relabel = relabels(key)
    head_ids = owned_ids(jax.random.fold_in(key, 1), relabel, EDGE_DEV)
    tail_ids = owned_ids(jax.random.fold_in(key, 2), relabel, EDGE_DEV)
    return jnp.stack([head_ids, tail_ids], axis=1).astype(jnp.int32)


def draw_negatives(key, part):
    relabel = relabels(key)
    return owned_ids(jax.random.fold_in(key, 3), relabel, NEG_DEV)


def touch_ends(values, key, least, top_value):
    shape = values.shape
    place = [jax.random.randint(jax.random.fold_in(key, axis), (), 0, shape[axis]) for axis in range(len(shape))]
    values = values.at[tuple(place)].set(least)
    longest = shape.index(max(shape))
    place[longest] = (place[longest] + 1) % shape[longest]
    return values.at[tuple(place)].set(top_value)


def level_of(stream_key, dims, cuts, low, top_value):
    level, own = 1.0, jax.random.fold_in(stream_key, 6)
    for axis_at, blocks in cuts:
        steps = jnp.exp(jax.random.uniform(jax.random.fold_in(own, axis_at), (blocks,), jnp.float32, low / len(cuts), top_value / len(cuts)))
        level = level * jnp.repeat(steps, dims[axis_at] // blocks).reshape([-1 if axis == axis_at else 1 for axis in range(len(dims))])
    return level


def rank_table(number_of, slope):
    loads = [(1 << 20) // math.isqrt(standing ** slope) + 1 for standing in range(1, number_of + 1)]
    scale = 1 + sum(loads) // (1 << 30)
    return np.cumsum(np.array([max(1, weight // scale) for weight in loads]))


def ranked(key, dims, amount, slope):
    table = rank_table(amount, slope)
    pick = jax.random.randint(jax.random.fold_in(key, 1), dims, 0, int(table[amount - 1]))
    rank = jnp.searchsorted(jnp.asarray(table, jnp.int32), pick, side="right")
    return jax.random.permutation(jax.random.fold_in(key, 2), amount)[rank].astype(jnp.int32)


def bell_draw(rng, extent, scale, limit, cuts=(), kind=jnp.bfloat16):
    entries = scale * jax.random.normal(rng, extent, jnp.float32)
    if cuts:
        entries = entries * level_of(rng, extent, cuts, -0.22, 0.18)
    return jnp.clip(entries, -limit, limit).astype(kind)


def setup_inputs(seed: int = 0) -> dict:
    seeds = jax.random.split(jax.random.key(seed), 8)
    return {
        "entities": bell_draw(seeds[0], (ENTITIES, DIM), 0.25, 1.5, ((0, 8),), jnp.float32),
        "entity_history": jnp.clip(jnp.exp(math.log(0.1) - 4.6051702 * jax.random.uniform(seeds[1], (ENTITIES,), jnp.float32) ** level_of(seeds[1], (ENTITIES,), ((0, 8),), -0.2, 0.2)), 0.001, 0.1),
        "relations": bell_draw(seeds[2], (RELS, DIM), 1.0, 6.0, (), jnp.float32),
        "relation_history": jnp.clip(jnp.exp(jax.random.uniform(seeds[3], (RELS,), jnp.float32, math.log(0.001), math.log(0.1))), 0.001, 0.1),
        "edge_ends": draw_edge_ends(jax.random.fold_in(seeds[7], 71), 0),
        "edge_relations": touch_ends(ranked(seeds[5], (EDGES,), RELS, 4), jax.random.fold_in(seeds[5], 3), 0, RELS - 1).astype(jnp.int32),
        "negatives": draw_negatives(jax.random.fold_in(seeds[7], 71), 0),
    }


learn_rate = 0.1
adagrad_eps = 1e-10

def halves(vectors):
    half_width = vectors.shape[-1] // 2
    return (vectors[..., :half_width], vectors[..., half_width:])

def complex_times(former, latter):
    former_real, former_imag = halves(former)
    latter_real, latter_imag = halves(latter)
    return jnp.concatenate([former_real * latter_real - former_imag * latter_imag, former_real * latter_imag + former_imag * latter_real], axis=-1)

def conjugate(vectors):
    real_part, imag_part = halves(vectors)
    return jnp.concatenate([real_part, -imag_part], axis=-1)

def side_loss(probe_rows, positive, candidates):
    scores = jnp.dot(probe_rows, candidates.T, precision=lax.Precision.HIGHEST)
    own_edge = jnp.arange(candidates.shape[0])[None, :] == jnp.arange(probe_rows.shape[0])[:, None]
    scores = jnp.where(own_edge, -jnp.inf, scores)
    joined = jnp.concatenate([positive[:, None], scores], axis=1)
    return jnp.sum(jax.nn.logsumexp(joined, axis=1) - positive)

def batch_loss(head_rows, related, tail_rows, negative_rows):
    tail_query = complex_times(head_rows, related)
    head_probe = complex_times(conjugate(related), tail_rows)
    positive = lax.optimization_barrier(jnp.sum(tail_query * tail_rows, axis=1))
    tail_side = side_loss(tail_query, positive, jnp.concatenate([tail_rows, negative_rows], axis=0))
    head_side = side_loss(head_probe, positive, jnp.concatenate([head_rows, negative_rows], axis=0))
    return tail_side + head_side

def adagrad_step(slope_vector, history):
    squares = history + lax.optimization_barrier(jnp.mean(slope_vector * slope_vector, axis=1))
    return (-learn_rate * slope_vector / (jnp.sqrt(squares)[:, None] + adagrad_eps), squares)

def reference(entities, entity_history, relations, relation_history, edge_ends, edge_relations, negatives):
    batches = EDGES // EDGE_DEV
    batched = (edge_ends.reshape(batches, EDGE_DEV, 2), edge_relations.reshape(batches, EDGE_DEV), negatives.reshape(batches, NEG_DEV))
    loss_grad = jax.value_and_grad(batch_loss, argnums=(0, 1, 2, 3))

    def advance(carried, pieces):
        entity_grad, relation_grad, summed = carried
        edge_pairs, relation_ids, negative_ids = pieces
        head_ids = edge_pairs[:, 0]
        tail_ids = edge_pairs[:, 1]
        loss_value, gradients = loss_grad(entities[head_ids], relations[relation_ids], entities[tail_ids], entities[negative_ids])
        entity_grad = entity_grad.at[head_ids].add(gradients[0])
        entity_grad = entity_grad.at[tail_ids].add(gradients[2])
        entity_grad = entity_grad.at[negative_ids].add(gradients[3])
        relation_grad = relation_grad.at[relation_ids].add(gradients[1])
        return ((entity_grad, relation_grad, summed + loss_value), None)
    initial = (jnp.zeros(entities.shape, jnp.float32), jnp.zeros(relations.shape, jnp.float32), jnp.zeros((), jnp.float32))
    finals, unused = lax.scan(advance, initial, batched)
    entity_grad, relation_grad, summed = finals
    entity_step, entity_squares = adagrad_step(entity_grad, entity_history)
    relation_step, relation_squares = adagrad_step(relation_grad, relation_history)
    mean_loss = (summed / (2 * EDGES)).reshape(1)
    return (entity_step, entity_squares, relation_step, relation_squares, mean_loss)
```

```python
import functools

import jax
import jax.numpy as jnp
from jax import lax
from jax.experimental import pallas as pl
from jax.experimental.pallas import tpu as pltpu
from jax.sharding import PartitionSpec as P

learn_rate = 0.1
adagrad_eps = 1e-10
highest = lax.Precision.HIGHEST


def halves(vectors):
    half_width = vectors.shape[-1] // 2
    return (vectors[..., :half_width], vectors[..., half_width:])


def complex_times(former, latter):
    former_real, former_imag = halves(former)
    latter_real, latter_imag = halves(latter)
    return jnp.concatenate(
        [
            former_real * latter_real - former_imag * latter_imag,
            former_real * latter_imag + former_imag * latter_real,
        ],
        axis=-1,
    )


def conjugate(vectors):
    real_part, imag_part = halves(vectors)
    return jnp.concatenate([real_part, -imag_part], axis=-1)


def adagrad_step(slope_vector, history):
    squares = history + jnp.mean(slope_vector * slope_vector, axis=1)
    return (-learn_rate * slope_vector / (jnp.sqrt(squares)[:, None] + adagrad_eps), squares)


def bucket_slots(node_labels, shard_rows, peer_count, room_limit):
    owners = node_labels // shard_rows
    local_rows = node_labels - owners * shard_rows
    onehot = (owners[:, None] == jnp.arange(peer_count, dtype=jnp.int32)[None, :]).astype(jnp.int32)
    earlier = jnp.cumsum(onehot, axis=0) - onehot
    slot_positions = owners * room_limit + jnp.sum(earlier * onehot, axis=1)
    request = jnp.full((peer_count * room_limit,), -1, jnp.int32).at[slot_positions].set(local_rows)
    return (slot_positions, request.reshape(peer_count, room_limit))


def serve_rows(table, demanded_lookups):
    picked = jnp.take(table, jnp.maximum(demanded_lookups, 0), axis=0)
    return jnp.where((demanded_lookups >= 0)[..., None], picked, 0.0)


def outgoing_rows(slope_vector, slot_positions, peer_count, room_limit):
    buffer_rows = (
        jnp.zeros((peer_count * room_limit, slope_vector.shape[1]), jnp.float32)
        .at[slot_positions]
        .set(slope_vector)
    )
    return buffer_rows.reshape(peer_count, room_limit, slope_vector.shape[1])


def absorb(dense_grad, demanded_lookups, incoming):
    flat_rows = jnp.maximum(demanded_lookups, 0).reshape(-1)
    return dense_grad.at[flat_rows].add(incoming.reshape(-1, incoming.shape[-1]))


def matmul(former, latter):
    return jnp.dot(former, latter, precision=highest, preferred_element_type=jnp.float32)


def spread_back(weights, probe_rows):
    return lax.dot_general(
        weights,
        probe_rows,
        (((0,), (0,)), ((), ())),
        precision=highest,
        preferred_element_type=jnp.float32,
    )


def side_terms(probe_rows, positive, candidates):
    scores = lax.dot_general(
        probe_rows,
        candidates,
        (((1,), (1,)), ((), ())),
        precision=highest,
        preferred_element_type=jnp.float32,
    )
    own_edge = lax.broadcasted_iota(jnp.int32, scores.shape, 1) == lax.broadcasted_iota(
        jnp.int32, scores.shape, 0
    )
    scores = jnp.where(own_edge, -jnp.inf, scores)
    peak = jnp.maximum(jnp.max(scores, axis=1), positive)
    lifted = jnp.exp(scores - peak[:, None])
    struck = jnp.exp(positive - peak)
    normal = struck + jnp.sum(lifted, axis=1)
    loss_sum = jnp.sum(jnp.log(normal) + peak - positive)
    return (loss_sum, lifted / normal[:, None], struck / normal)


def on_device(
    entities, entity_history, relations, relation_history, edge_ends, edge_relations, negatives
):
    peer_count = lax.axis_size("ea")
    shard_rows = entities.shape[0]
    row_width = entities.shape[1]
    edge_count = edge_ends.shape[0]
    negative_count = negatives.shape[0]
    edge_share = edge_count // peer_count
    link_room = edge_share + max(1, edge_share // 2)
    negative_share = negative_count // peer_count
    contrast_room = negative_share + max(1, negative_share // 2)
    desired_items = (edge_ends[:, 0], edge_ends[:, 1], negatives)
    room_limits = (link_room, link_room, contrast_room)
    joint_capacity = sum(room_limits)
    joint_places, joint_request = bucket_slots(
        jnp.concatenate(desired_items), shard_rows, peer_count, joint_capacity
    )
    joint_asked = lax.all_to_all(joint_request, "ea", split_axis=0, concat_axis=0, tiled=True)
    joint_answer = lax.all_to_all(
        serve_rows(entities, joint_asked), "ea", split_axis=0, concat_axis=0, tiled=True
    )
    fetched = joint_answer.reshape(-1, row_width)[joint_places]
    head_rows = fetched[:edge_count]
    tail_rows = fetched[edge_count : 2 * edge_count]
    negative_rows = fetched[2 * edge_count :]
    related = jnp.take(relations, edge_relations, axis=0)
    tail_query = complex_times(head_rows, related)
    head_probe = complex_times(conjugate(related), tail_rows)
    positive = jnp.sum(tail_query * tail_rows, axis=1)
    tail_cands = jnp.concatenate([tail_rows, negative_rows], axis=0)
    head_cands = jnp.concatenate([head_rows, negative_rows], axis=0)
    tail_loss, tail_weight, tail_struck = side_terms(tail_query, positive, tail_cands)
    head_loss, head_weight, head_struck = side_terms(head_probe, positive, head_cands)
    gain = tail_struck + head_struck - 2.0
    tail_back = matmul(tail_weight, tail_cands) + gain[:, None] * tail_rows
    head_back = matmul(head_weight, head_cands)
    tail_spread = spread_back(tail_weight, tail_query)
    head_spread = spread_back(head_weight, head_probe)
    head_grad = complex_times(tail_back, conjugate(related)) + head_spread[:edge_count]
    tail_grad = (
        gain[:, None] * tail_query + complex_times(head_back, related) + tail_spread[:edge_count]
    )
    negative_grad = tail_spread[edge_count:] + head_spread[edge_count:]
    relation_rows = complex_times(tail_back, conjugate(head_rows)) + complex_times(
        conjugate(head_back), tail_rows
    )
    relation_local = jax.ops.segment_sum(
        relation_rows, edge_relations, num_segments=relations.shape[0]
    )
    loss_local = tail_loss + head_loss
    dense_grad = jnp.zeros((shard_rows, row_width), jnp.float32)
    joint_grad = jnp.concatenate([head_grad, tail_grad, negative_grad], axis=0)
    incoming = lax.all_to_all(
        outgoing_rows(joint_grad, joint_places, peer_count, joint_capacity),
        "ea",
        split_axis=0,
        concat_axis=0,
        tiled=True,
    )
    dense_grad = absorb(dense_grad, joint_asked, incoming)
    relation_sum, loss_sum = lax.psum((relation_local, loss_local), ("ea", "ba"))
    relation_step, relation_squares = adagrad_step(relation_sum, relation_history)
    mean_loss = (loss_sum / (2.0 * edge_count * peer_count * lax.axis_size("ba"))).reshape(1)
    summed = lax.psum(dense_grad, "ba")
    entity_step, entity_squares = adagrad_step(summed, entity_history)
    return (entity_step, entity_squares, relation_step, relation_squares, mean_loss)


LANES = 128
TAIL_ROWS = 16
MESH = pl.DeviceIdType.MESH
f32 = jnp.float32


def split_two(values):
    upper = values.astype(jnp.bfloat16)
    return upper, (values - upper.astype(f32)).astype(jnp.bfloat16)


def dot_of(former, latter, dims):
    return lax.dot_general(former, latter, (dims, ((), ())), preferred_element_type=f32)


def dot_three(former, latter, dims):
    return dot_of(former[0], latter[0], dims) + (
        dot_of(former[0], latter[1], dims) + dot_of(former[1], latter[0], dims)
    )


def pick_rows(onehot, halves_of):
    dims = ((1,), (0,))
    return dot_of(onehot, halves_of[0], dims) + dot_of(onehot, halves_of[1], dims)


def times(former, latter):
    a, b = former[:, :LANES], former[:, LANES:]
    c, d = latter[:, :LANES], latter[:, LANES:]
    return jnp.concatenate([a * c - b * d, a * d + b * c], axis=1)


def times_conj(former, latter):
    a, b = former[:, :LANES], former[:, LANES:]
    c, d = latter[:, :LANES], latter[:, LANES:]
    return jnp.concatenate([a * c + b * d, b * c - a * d], axis=1)


def one_side(probe, positive, cands):
    probe_parts, cand_parts = split_two(probe), split_two(cands)
    scores = dot_three(probe_parts, cand_parts, ((1,), (1,)))
    own = lax.broadcasted_iota(jnp.int32, scores.shape, 1) == lax.broadcasted_iota(
        jnp.int32, scores.shape, 0
    )
    scores = jnp.where(own, -jnp.inf, scores)
    peak = jnp.maximum(jnp.max(scores, axis=1, keepdims=True), positive)
    lifted = jnp.exp(scores - peak)
    struck = jnp.exp(positive - peak)
    normal = struck + jnp.sum(lifted, axis=1, keepdims=True)
    loss = jnp.sum(jnp.log(normal) + peak - positive, axis=0, keepdims=True)
    weight = split_two(lifted / normal)
    back = dot_three(weight, cand_parts, ((1,), (0,)))
    spread = dot_three(weight, probe_parts, ((0,), (0,)))
    return loss, struck / normal, back, spread


def step_kernel(
    n,
    ids_col,
    ids_row,
    kinds_col,
    kinds_row,
    ent,
    rels,
    sum_out,
    rel_out,
    loss_out,
    tab,
    rows,
    grad_hi,
    grad_lo,
    rel_local,
    loss_local,
    pbuf,
    dbuf,
    rbuf,
    fin,
    xbuf,
    full,
    relbuf,
    ag_send,
    ag_recv,
    pair_send,
    pair_recv,
    rs_send,
    rs_recv,
    half_send,
    half_recv,
    last_send,
    last_recv,
    rel_send,
    rel_recv,
):
    mid = n // 2
    shard = ent.shape[0]
    edges = kinds_col.shape[0]
    reads = ids_col.shape[0]
    rel_share = rels.shape[0] // n
    chunk = pbuf.shape[1]
    me = lax.axis_index("ea")
    lane = lax.axis_index("ba")
    core = lax.rem(lane, 2)

    def at(place):
        place = lax.rem(place + 2 * n, n)
        return 2 * place + (place // mid) * (2 * (n - place) - 1 - 2 * place)

    high, odd = me // 2, lax.rem(me, 2)
    pos = high + odd * (n - 1 - 2 * high)
    onward = ({"ea": at(pos + 1)}, {"ea": at(pos - 1)})
    partner = {"ba": lane + 1 - 2 * core}
    across = {"ba": lax.rem(lane + 2, 4)}

    barrier = pltpu.get_barrier_semaphore()
    for j in range(1, n):
        pl.semaphore_signal(barrier, inc=1, device_id={"ea": lax.rem(me + j, n)}, device_id_type=MESH)
    pl.semaphore_signal(barrier, inc=1, device_id=partner, device_id_type=MESH)
    pl.semaphore_signal(barrier, inc=1, device_id=across, device_id_type=MESH)
    pl.semaphore_wait(barrier, n + 1)

    sent = []

    def send(src, dst, send_sem, recv_sem, device):
        return pltpu.make_async_remote_copy(
            src_ref=src, dst_ref=dst, send_sem=send_sem, recv_sem=recv_sem,
            device_id=device, device_id_type=MESH,
        )

    def launch(copy):
        copy.start()
        sent.append(copy)

    sub = shard // 4

    def ag_rows(u):
        return pl.ds(pl.multiple_of(core * (2 * sub) + u * sub, 8), sub)

    def ag_active(d, s, u):
        return s < mid or (s == mid and u == d)

    def ag_copy(d, s, u):
        source = (s - 1) if d == 0 else (n - (s - 1)) % n
        target = s if d == 0 else n - s
        src = ent.at[ag_rows(u)] if s == 1 else tab.at[source, ag_rows(u)]
        return send(src, tab.at[target, ag_rows(u)], ag_send.at[d, s - 1, u], ag_recv.at[d, s - 1, u], onward[d])

    def pair_copy(slot, u):
        return send(tab.at[slot, ag_rows(u)], tab.at[slot, ag_rows(u)], pair_send.at[slot, u], pair_recv.at[slot, u], partner)

    def gather(slot):
        values = ent[...] if slot == 0 else tab[slot]
        owner = at(pos - slot)
        onehot = (ids_col[...] - owner * shard == lax.broadcasted_iota(jnp.int32, (reads, shard), 1)).astype(f32).astype(jnp.bfloat16)
        picked = pick_rows(onehot, split_two(values))
        if slot == 0:
            rows[...] = picked
        else:
            rows[...] += picked

    for u in range(2):
        for d in range(2):
            launch(ag_copy(d, 1, u if d == 0 else 1 - u))
    gather(0)
    kinds = (kinds_col[...] == lax.broadcasted_iota(jnp.int32, (edges, rels.shape[0]), 1)).astype(f32).astype(jnp.bfloat16)
    related = pick_rows(kinds, split_two(rels[...]))
    slots_of = lambda s: (s, n - s) if s < mid else (s,)
    for s in range(1, mid + 1):
        for v in range(2):
            for d in range(2):
                u = v if d == 0 else 1 - v
                if ag_active(d, s, u):
                    ag_copy(d, s, u).wait_recv()
                    if s < mid and ag_active(d, s + 1, u):
                        launch(ag_copy(d, s + 1, u))
                    launch(pair_copy(s if d == 0 else n - s, u))
        if s > 1:
            for slot in slots_of(s - 1):
                for u in range(2):
                    pair_copy(slot, u).wait_recv()
                gather(slot)
    for u in range(2):
        pair_copy(mid, u).wait_recv()
    gather(mid)

    head, tail, contrast = rows[:edges], rows[edges : 2 * edges], rows[2 * edges :]
    query = times(head, related)
    probe = times_conj(tail, related)
    positive = jnp.sum(query * tail, axis=1, keepdims=True)
    tail_loss, tail_struck, tail_back, tail_spread = one_side(query, positive, jnp.concatenate([tail, contrast], axis=0))
    head_loss, head_struck, head_back, head_spread = one_side(probe, positive, jnp.concatenate([head, contrast], axis=0))
    gain = tail_struck + head_struck - 2.0
    tail_back = tail_back + gain * tail
    grads = (
        times_conj(tail_back, related) + head_spread[:edges],
        gain * query + times(head_back, related) + tail_spread[:edges],
        tail_spread[edges:] + head_spread[edges:],
    )
    start = 0
    for part in grads:
        upper, lower = split_two(part)
        grad_hi[start : start + part.shape[0]] = upper
        grad_lo[start : start + part.shape[0]] = lower
        start += part.shape[0]
    rel_rows = times_conj(tail_back, head) + times_conj(tail, head_back)
    kinds_t = (kinds_row[...] == lax.broadcasted_iota(jnp.int32, (rels.shape[0], edges), 0)).astype(f32).astype(jnp.bfloat16)
    rel_local[...] = pick_rows(kinds_t, split_two(rel_rows))
    corner = (lax.broadcasted_iota(jnp.int32, loss_local.shape, 0) == 0) & (
        lax.broadcasted_iota(jnp.int32, loss_local.shape, 1) == 0
    )
    loss_local[...] = jnp.where(corner, tail_loss + head_loss, 0.0)

    half = chunk // 2
    cut = (half // 16) * 8
    mine = pl.multiple_of(core * half, 8)
    other = pl.multiple_of((1 - core) * half, 8)
    spans = ((0, cut), (cut, half - cut))

    def half_copy(k):
        return send(pbuf.at[k, pl.ds(other, half)], dbuf.at[k], half_send.at[k], half_recv.at[k], partner)

    def contribute(k):
        owner = at(pos + k)
        onehot = (ids_row[...] - owner * shard == lax.broadcasted_iota(jnp.int32, (shard, reads), 0)).astype(f32).astype(jnp.bfloat16)
        pbuf[k, :shard] = pick_rows(onehot, (grad_hi[...], grad_lo[...]))
        pbuf[k, shard : shard + rel_share] = rel_local[pl.ds(pl.multiple_of(owner * rel_share, 8), rel_share)]
        pbuf[k, shard + rel_share :] = loss_local[...]
        launch(half_copy(k))

    def rs_active(d, s, u):
        return s > 1 or u == d

    def rs_copy(d, s, u):
        k = (mid + 1 - s) if d == 0 else n - (mid + 1 - s)
        low, size = spans[u]
        return send(
            pbuf.at[k, pl.ds(pl.multiple_of(mine + low, 8), size)],
            rbuf.at[d, s - 1, pl.ds(low, size)],
            rs_send.at[d, s - 1, u],
            rs_recv.at[d, s - 1, u],
            onward[d],
        )

    chunks_at = lambda s: (mid,) if s == 1 else (mid + 1 - s, n - (mid + 1 - s)) if s <= mid else (0,)
    for s in (1, 2):
        for k in chunks_at(s):
            contribute(k)
    for s in range(1, mid + 1):
        for k in chunks_at(s):
            half_copy(k).wait_recv()
        for v in range(2):
            for d in range(2):
                u = (1 - d) if v == 0 else d
                if not rs_active(d, s, u):
                    continue
                k = (mid + 1 - s) if d == 0 else n - (mid + 1 - s)
                low, size = spans[u]
                here = pl.ds(pl.multiple_of(mine + low, 8), size)
                total = pbuf[k, here] + dbuf[k, pl.ds(low, size)]
                if s > 1 and rs_active(d, s - 1, u):
                    rs_copy(d, s - 1, u).wait_recv()
                    total = total + rbuf[d, s - 2, pl.ds(low, size)]
                pbuf[k, here] = total
                launch(rs_copy(d, s, u))
        if s + 2 <= mid + 1:
            for k in chunks_at(s + 2):
                contribute(k)
    half_copy(0).wait_recv()

    def last_copy(stage, u):
        low, size = spans[u]
        if stage == 0:
            return send(fin.at[pl.ds(low, size)], xbuf.at[pl.ds(low, size)], last_send.at[0, u], last_recv.at[0, u], across)
        here = pl.ds(pl.multiple_of(mine + low, 8), size)
        return send(full.at[here], full.at[here], last_send.at[1, u], last_recv.at[1, u], partner)

    for u in (1, 0):
        low, size = spans[u]
        total = pbuf[0, pl.ds(pl.multiple_of(mine + low, 8), size)] + dbuf[0, pl.ds(low, size)]
        for d in range(2):
            rs_copy(d, mid, u).wait_recv()
            total = total + rbuf[d, mid - 1, pl.ds(low, size)]
        fin[pl.ds(low, size)] = total
        launch(last_copy(0, u))
    for u in (1, 0):
        low, size = spans[u]
        last_copy(0, u).wait_recv()
        full[pl.ds(pl.multiple_of(mine + low, 8), size)] = fin[pl.ds(low, size)] + xbuf[pl.ds(low, size)]
        launch(last_copy(1, u))
    for u in (1, 0):
        last_copy(1, u).wait_recv()

    def rel_copy(j):
        return send(full.at[pl.ds(shard, rel_share)], relbuf.at[j], rel_send.at[j], rel_recv.at[j], {"ea": lax.rem(me + j, n)})

    for j in range(1, n):
        launch(rel_copy(j))
    sum_out[...] = full[:shard]
    loss_out[...] = full[shard + rel_share : shard + rel_share + 8, :LANES]
    rel_out[pl.ds(pl.multiple_of(me * rel_share, 8), rel_share)] = full[shard : shard + rel_share]
    for j in range(1, n):
        rel_copy(j).wait_recv()
        source = lax.rem(me - j + n, n)
        rel_out[pl.ds(pl.multiple_of(source * rel_share, 8), rel_share)] = relbuf[j]
    for copy in sent:
        copy.wait_send()


def spread_halves(values):
    half = values.shape[1] // 2
    pad = jnp.zeros((values.shape[0], LANES - half), values.dtype)
    return jnp.concatenate([values[:, :half], pad, values[:, half:], pad], axis=1)


def join_halves(values, width):
    half = width // 2
    return jnp.concatenate([values[:, :half], values[:, LANES : LANES + half]], axis=1)


def on_ring(entities, entity_history, relations, relation_history, edge_ends, edge_relations, negatives):
    n = lax.axis_size("ea")
    shard, width = entities.shape
    rel_count = relations.shape[0]
    edges = edge_ends.shape[0]
    ids = jnp.concatenate([edge_ends[:, 0], edge_ends[:, 1], negatives])
    reads = ids.shape[0]
    chunk = shard + rel_count // n + TAIL_ROWS
    wide = 2 * LANES
    mid = n // 2
    dma = pltpu.SemaphoreType.DMA
    vmem = pl.BlockSpec(memory_space=pltpu.VMEM)
    summed, rel_sum, loss = pl.pallas_call(
        functools.partial(step_kernel, n),
        out_shape=(
            jax.ShapeDtypeStruct((shard, wide), f32),
            jax.ShapeDtypeStruct((rel_count, wide), f32),
            jax.ShapeDtypeStruct((8, LANES), f32),
        ),
        in_specs=[vmem] * 6,
        out_specs=(vmem,) * 3,
        scratch_shapes=[
            pltpu.VMEM((n, shard, wide), f32),
            pltpu.VMEM((reads, wide), f32),
            pltpu.VMEM((reads, wide), jnp.bfloat16),
            pltpu.VMEM((reads, wide), jnp.bfloat16),
            pltpu.VMEM((rel_count, wide), f32),
            pltpu.VMEM((TAIL_ROWS, wide), f32),
            pltpu.VMEM((n, chunk, wide), f32),
            pltpu.VMEM((n, chunk // 2, wide), f32),
            pltpu.VMEM((2, mid, chunk // 2, wide), f32),
            pltpu.VMEM((chunk // 2, wide), f32),
            pltpu.VMEM((chunk // 2, wide), f32),
            pltpu.VMEM((chunk, wide), f32),
            pltpu.VMEM((n, rel_count // n, wide), f32),
            dma((2, mid, 2)),
            dma((2, mid, 2)),
            dma((n, 2)),
            dma((n, 2)),
            dma((2, mid, 2)),
            dma((2, mid, 2)),
            dma((n,)),
            dma((n,)),
            dma((2, 2)),
            dma((2, 2)),
            dma((n,)),
            dma((n,)),
        ],
        compiler_params=pltpu.CompilerParams(
            collective_id=0, has_side_effects=True, vmem_limit_bytes=60 * 1024 * 1024
        ),
    )(
        ids[:, None],
        ids[None, :],
        edge_relations[:, None],
        edge_relations[None, :],
        spread_halves(entities),
        spread_halves(relations),
    )
    relation_step, relation_squares = adagrad_step(join_halves(rel_sum, width), relation_history)
    entity_step, entity_squares = adagrad_step(join_halves(summed, width), entity_history)
    mean_loss = (loss[0, 0] / (2.0 * edges * n * lax.axis_size("ba"))).reshape(1)
    return (entity_step, entity_squares, relation_step, relation_squares, mean_loss)


def fits_ring(mesh):
    n = mesh.shape["ea"]
    return mesh.shape["ba"] == 4 and n % 2 == 0 and 4 <= n <= 16


def solution(mesh):
    placed = (
        P("ea", None),
        P("ea"),
        P(),
        P(),
        P(("ba", "ea"), None),
        P(("ba", "ea")),
        P(("ba", "ea")),
    )
    return jax.shard_map(
        on_ring if fits_ring(mesh) else on_device,
        mesh=mesh,
        in_specs=placed,
        out_specs=(P("ea", None), P("ea"), P(), P(), P()),
        check_vma=False,
    )
```

```python
import functools

import jax
import jax.numpy as jnp
from jax import lax
from jax.experimental import pallas as pl
from jax.experimental.pallas import tpu as pltpu
from jax.sharding import PartitionSpec as P

learn_rate = 0.1
adagrad_eps = 1e-10
highest = lax.Precision.HIGHEST


def halves(vectors):
    half_width = vectors.shape[-1] // 2
    return (vectors[..., :half_width], vectors[..., half_width:])


def complex_times(former, latter):
    former_real, former_imag = halves(former)
    latter_real, latter_imag = halves(latter)
    return jnp.concatenate(
        [
            former_real * latter_real - former_imag * latter_imag,
            former_real * latter_imag + former_imag * latter_real,
        ],
        axis=-1,
    )


def conjugate(vectors):
    real_part, imag_part = halves(vectors)
    return jnp.concatenate([real_part, -imag_part], axis=-1)


def adagrad_step(slope_vector, history):
    squares = history + jnp.mean(slope_vector * slope_vector, axis=1)
    return (-learn_rate * slope_vector / (jnp.sqrt(squares)[:, None] + adagrad_eps), squares)


def bucket_slots(node_labels, shard_rows, peer_count, room_limit):
    owners = node_labels // shard_rows
    local_rows = node_labels - owners * shard_rows
    onehot = (owners[:, None] == jnp.arange(peer_count, dtype=jnp.int32)[None, :]).astype(jnp.int32)
    earlier = jnp.cumsum(onehot, axis=0) - onehot
    slot_positions = owners * room_limit + jnp.sum(earlier * onehot, axis=1)
    request = jnp.full((peer_count * room_limit,), -1, jnp.int32).at[slot_positions].set(local_rows)
    return (slot_positions, request.reshape(peer_count, room_limit))


def serve_rows(table, demanded_lookups):
    picked = jnp.take(table, jnp.maximum(demanded_lookups, 0), axis=0)
    return jnp.where((demanded_lookups >= 0)[..., None], picked, 0.0)


def outgoing_rows(slope_vector, slot_positions, peer_count, room_limit):
    buffer_rows = (
        jnp.zeros((peer_count * room_limit, slope_vector.shape[1]), jnp.float32)
        .at[slot_positions]
        .set(slope_vector)
    )
    return buffer_rows.reshape(peer_count, room_limit, slope_vector.shape[1])


def absorb(dense_grad, demanded_lookups, incoming):
    flat_rows = jnp.maximum(demanded_lookups, 0).reshape(-1)
    return dense_grad.at[flat_rows].add(incoming.reshape(-1, incoming.shape[-1]))


def matmul(former, latter):
    return jnp.dot(former, latter, precision=highest, preferred_element_type=jnp.float32)


def spread_back(weights, probe_rows):
    return lax.dot_general(
        weights,
        probe_rows,
        (((0,), (0,)), ((), ())),
        precision=highest,
        preferred_element_type=jnp.float32,
    )


def side_terms(probe_rows, positive, candidates):
    scores = lax.dot_general(
        probe_rows,
        candidates,
        (((1,), (1,)), ((), ())),
        precision=highest,
        preferred_element_type=jnp.float32,
    )
    own_edge = lax.broadcasted_iota(jnp.int32, scores.shape, 1) == lax.broadcasted_iota(
        jnp.int32, scores.shape, 0
    )
    scores = jnp.where(own_edge, -jnp.inf, scores)
    peak = jnp.maximum(jnp.max(scores, axis=1), positive)
    lifted = jnp.exp(scores - peak[:, None])
    struck = jnp.exp(positive - peak)
    normal = struck + jnp.sum(lifted, axis=1)
    loss_sum = jnp.sum(jnp.log(normal) + peak - positive)
    return (loss_sum, lifted / normal[:, None], struck / normal)


def on_device(
    entities, entity_history, relations, relation_history, edge_ends, edge_relations, negatives
):
    peer_count = lax.axis_size("ea")
    shard_rows = entities.shape[0]
    row_width = entities.shape[1]
    edge_count = edge_ends.shape[0]
    negative_count = negatives.shape[0]
    edge_share = edge_count // peer_count
    link_room = edge_share + max(1, edge_share // 2)
    negative_share = negative_count // peer_count
    contrast_room = negative_share + max(1, negative_share // 2)
    desired_items = (edge_ends[:, 0], edge_ends[:, 1], negatives)
    room_limits = (link_room, link_room, contrast_room)
    joint_capacity = sum(room_limits)
    joint_places, joint_request = bucket_slots(
        jnp.concatenate(desired_items), shard_rows, peer_count, joint_capacity
    )
    joint_asked = lax.all_to_all(joint_request, "ea", split_axis=0, concat_axis=0, tiled=True)
    joint_answer = lax.all_to_all(
        serve_rows(entities, joint_asked), "ea", split_axis=0, concat_axis=0, tiled=True
    )
    fetched = joint_answer.reshape(-1, row_width)[joint_places]
    head_rows = fetched[:edge_count]
    tail_rows = fetched[edge_count : 2 * edge_count]
    negative_rows = fetched[2 * edge_count :]
    related = jnp.take(relations, edge_relations, axis=0)
    tail_query = complex_times(head_rows, related)
    head_probe = complex_times(conjugate(related), tail_rows)
    positive = jnp.sum(tail_query * tail_rows, axis=1)
    tail_cands = jnp.concatenate([tail_rows, negative_rows], axis=0)
    head_cands = jnp.concatenate([head_rows, negative_rows], axis=0)
    tail_loss, tail_weight, tail_struck = side_terms(tail_query, positive, tail_cands)
    head_loss, head_weight, head_struck = side_terms(head_probe, positive, head_cands)
    gain = tail_struck + head_struck - 2.0
    tail_back = matmul(tail_weight, tail_cands) + gain[:, None] * tail_rows
    head_back = matmul(head_weight, head_cands)
    tail_spread = spread_back(tail_weight, tail_query)
    head_spread = spread_back(head_weight, head_probe)
    head_grad = complex_times(tail_back, conjugate(related)) + head_spread[:edge_count]
    tail_grad = (
        gain[:, None] * tail_query + complex_times(head_back, related) + tail_spread[:edge_count]
    )
    negative_grad = tail_spread[edge_count:] + head_spread[edge_count:]
    relation_rows = complex_times(tail_back, conjugate(head_rows)) + complex_times(
        conjugate(head_back), tail_rows
    )
    relation_local = jax.ops.segment_sum(
        relation_rows, edge_relations, num_segments=relations.shape[0]
    )
    loss_local = tail_loss + head_loss
    dense_grad = jnp.zeros((shard_rows, row_width), jnp.float32)
    joint_grad = jnp.concatenate([head_grad, tail_grad, negative_grad], axis=0)
    incoming = lax.all_to_all(
        outgoing_rows(joint_grad, joint_places, peer_count, joint_capacity),
        "ea",
        split_axis=0,
        concat_axis=0,
        tiled=True,
    )
    dense_grad = absorb(dense_grad, joint_asked, incoming)
    relation_sum, loss_sum = lax.psum((relation_local, loss_local), ("ea", "ba"))
    relation_step, relation_squares = adagrad_step(relation_sum, relation_history)
    mean_loss = (loss_sum / (2.0 * edge_count * peer_count * lax.axis_size("ba"))).reshape(1)
    summed = lax.psum(dense_grad, "ba")
    entity_step, entity_squares = adagrad_step(summed, entity_history)
    return (entity_step, entity_squares, relation_step, relation_squares, mean_loss)


LANES = 128
MESH = pl.DeviceIdType.MESH
f32 = jnp.float32


def split_two(values):
    upper = values.astype(jnp.bfloat16)
    return upper, (values - upper.astype(f32)).astype(jnp.bfloat16)


def dot_of(former, latter, dims):
    return lax.dot_general(former, latter, (dims, ((), ())), preferred_element_type=f32)


def dot_three(former, latter, dims):
    return dot_of(former[0], latter[0], dims) + (
        dot_of(former[0], latter[1], dims) + dot_of(former[1], latter[0], dims)
    )


def pick_rows(onehot, halves_of):
    dims = ((1,), (0,))
    return dot_of(onehot, halves_of[0], dims) + dot_of(onehot, halves_of[1], dims)


def times(former, latter):
    a, b = former[:, :LANES], former[:, LANES:]
    c, d = latter[:, :LANES], latter[:, LANES:]
    return jnp.concatenate([a * c - b * d, a * d + b * c], axis=1)


def times_conj(former, latter):
    a, b = former[:, :LANES], former[:, LANES:]
    c, d = latter[:, :LANES], latter[:, LANES:]
    return jnp.concatenate([a * c + b * d, b * c - a * d], axis=1)


def one_side(probe, positive, cands):
    probe_parts, cand_parts = split_two(probe), split_two(cands)
    scores = dot_three(probe_parts, cand_parts, ((1,), (1,)))
    own = lax.broadcasted_iota(jnp.int32, scores.shape, 1) == lax.broadcasted_iota(
        jnp.int32, scores.shape, 0
    )
    scores = jnp.where(own, -jnp.inf, scores)
    peak = jnp.maximum(jnp.max(scores, axis=1, keepdims=True), positive)
    lifted = jnp.exp(scores - peak)
    struck = jnp.exp(positive - peak)
    normal = struck + jnp.sum(lifted, axis=1, keepdims=True)
    loss = jnp.sum(jnp.log(normal) + peak - positive, axis=0, keepdims=True)
    weight = split_two(lifted / normal)
    back = dot_three(weight, cand_parts, ((1,), (0,)))
    spread = dot_three(weight, probe_parts, ((0,), (0,)))
    return loss, struck / normal, back, spread


def lanes_of(values):
    return lax.broadcasted_iota(jnp.int32, values.shape, 1)


def pack_extra(extra, width):
    count = extra.shape[0]
    mid_lane = LANES // 2
    narrow = width - LANES - mid_lane
    groups = LANES // narrow
    low, high = extra[: count // 2], extra[count // 2 :]
    broad = jnp.where(lanes_of(low) < mid_lane, low, pltpu.roll(high, mid_lane, 1))
    step = count // groups
    thin = jnp.zeros((step, LANES), f32)
    group_at = lanes_of(thin) // narrow
    for g in range(groups):
        moved = pltpu.roll(extra[g * step : (g + 1) * step], (g * narrow + mid_lane) % LANES, 1)
        thin = jnp.where(group_at == g, moved, thin)
    return broad, thin


def unpack_extra(broad, thin, width):
    mid_lane = LANES // 2
    narrow = width - LANES - mid_lane
    groups = LANES // narrow
    from_broad = jnp.concatenate([broad, pltpu.roll(broad, mid_lane, 1)], axis=0)
    turned = [
        thin if (mid_lane - g * narrow) % LANES == 0 else pltpu.roll(thin, (mid_lane - g * narrow) % LANES, 1)
        for g in range(groups)
    ]
    from_thin = jnp.concatenate(turned, axis=0)
    lanes = lanes_of(from_broad)
    return jnp.where(lanes < mid_lane, from_broad, jnp.where(lanes < width - LANES, from_thin, 0.0))


def to_halves(natural, width):
    half = width // 2
    shift = LANES - half
    base, extra = natural[:, :LANES], natural[:, LANES:]
    lanes = lanes_of(base)
    real = jnp.where(lanes < half, base, 0.0)
    imag = jnp.where(lanes < shift, pltpu.roll(base, shift, 1), jnp.where(lanes < half, pltpu.roll(extra, shift, 1), 0.0))
    return jnp.concatenate([real, imag], axis=1)


def to_natural(halved, width):
    half = width // 2
    turned = pltpu.roll(halved[:, LANES:], half, 1)
    lanes = lanes_of(turned)
    base = jnp.where(lanes < half, halved[:, :LANES], turned)
    return jnp.concatenate([base, jnp.where(lanes < width - LANES, turned, 0.0)], axis=1)


def update_of(base, extra, history, width):
    extra = jnp.where(lanes_of(extra) < width - LANES, extra, 0.0)
    mean = jnp.sum(base * base + extra * extra, axis=1, keepdims=True) / width
    squares = history + mean
    scale = -learn_rate / (jnp.sqrt(squares) + adagrad_eps)
    return base * scale, extra * scale, squares


def step_kernel(
    n,
    ag_sizes,
    rs_sizes,
    ids_col,
    ids_row,
    kinds_col,
    kinds_row,
    ent,
    ent_hist,
    rels,
    rel_hist,
    ent_out,
    ent_sq_out,
    rel_out,
    rel_sq_out,
    loss_out,
    tab,
    wide_buf,
    rows,
    grad_hi,
    grad_lo,
    rel_local,
    pbuf,
    dbuf,
    abuf,
    rbuf,
    fin,
    xbuf,
    full,
    relbuf,
    ag_send,
    ag_recv,
    pair_send,
    pair_recv,
    cross_send,
    cross_recv,
    rs_send,
    rs_recv,
    half_send,
    half_recv,
    over_send,
    over_recv,
    last_send,
    last_recv,
    rel_send,
    rel_recv,
):
    mid = n // 2
    shard, width = ent.shape
    rel_count = rels.shape[0]
    edges = kinds_col.shape[0]
    reads = ids_col.shape[0]
    rel_share = rel_count // n
    packed = tab.shape[1]
    broad_at, thin_at = shard, shard + shard // 2
    me = lax.axis_index("ea")
    lane = lax.axis_index("ba")
    core = lax.rem(lane, 2)
    plane = lane // 2

    def at(place):
        place = lax.rem(place + 2 * n, n)
        return 2 * place + (place // mid) * (2 * (n - place) - 1 - 2 * place)

    high, odd = me // 2, lax.rem(me, 2)
    pos = high + odd * (n - 1 - 2 * high)
    onward = ({"ea": at(pos + 1)}, {"ea": at(pos - 1)})
    partner = {"ba": lane + 1 - 2 * core}
    across = {"ba": lax.rem(lane + 2, 4)}

    barrier = pltpu.get_barrier_semaphore()
    for j in range(1, n):
        pl.semaphore_signal(barrier, inc=1, device_id={"ea": lax.rem(me + j, n)}, device_id_type=MESH)
    pl.semaphore_signal(barrier, inc=1, device_id=partner, device_id_type=MESH)
    pl.semaphore_signal(barrier, inc=1, device_id=across, device_id_type=MESH)

    wide_buf[...] = jnp.zeros_like(wide_buf)
    wide_buf[:shard, : width - LANES] = ent[:, LANES:]
    tab[0, :shard] = ent[:, :LANES]
    broad, thin = pack_extra(wide_buf[:shard], width)
    tab[0, broad_at:thin_at] = broad
    tab[0, thin_at:] = thin
    pl.semaphore_wait(barrier, n + 1)

    sent = []

    def send(src, dst, send_sem, recv_sem, device):
        return pltpu.make_async_remote_copy(
            src_ref=src, dst_ref=dst, send_sem=send_sem, recv_sem=recv_sem,
            device_id=device, device_id_type=MESH,
        )

    def launch(copy):
        copy.start()
        sent.append(copy)

    def span(sizes, which_core, u):
        base, cross = sizes
        start = which_core * (base + 2 * cross)
        if u == 0:
            return pl.ds(pl.multiple_of(start, 8), base)
        chosen = plane if u == 1 else 1 - plane
        return pl.ds(pl.multiple_of(start + base + chosen * cross, 8), cross)

    def ag_active(d, s, u):
        return s < mid or (s == mid and u == d)

    def ag_copy(d, s, u):
        source = (s - 1) if d == 0 else (n - (s - 1)) % n
        target = s if d == 0 else n - s
        where = span(ag_sizes, core, u)
        return send(tab.at[source, where], tab.at[target, where], ag_send.at[d, s - 1, u], ag_recv.at[d, s - 1, u], onward[d])

    def pair_copy(slot, u):
        where = tab.at[slot, span(ag_sizes, core, u)]
        return send(where, where, pair_send.at[slot, u], pair_recv.at[slot, u], partner)

    def cross_copy(slot):
        where = tab.at[slot, span(ag_sizes, core, 1)]
        return send(where, where, cross_send.at[slot], cross_recv.at[slot], across)

    def relay(slot):
        cross_copy(slot).wait_recv()
        launch(pair_copy(slot, 2))

    def gather(slot):
        owner = at(pos - slot)
        onehot = (ids_col[...] - owner * shard == lax.broadcasted_iota(jnp.int32, (reads, shard), 1)).astype(f32).astype(jnp.bfloat16)
        if slot:
            for u in range(3):
                pair_copy(slot, u).wait_recv()
            extra = unpack_extra(tab[slot, broad_at:thin_at], tab[slot, thin_at:], width)
        else:
            extra = wide_buf[:shard]
        picked = pick_rows(onehot, split_two(jnp.concatenate([tab[slot, :shard], extra], axis=1)))
        if slot:
            rows[...] += picked
        else:
            rows[...] = picked

    for v in range(2):
        for d in range(2):
            launch(ag_copy(d, 1, v if d == 0 else 1 - v))
    gather(0)
    wide_buf[:rel_count, : width - LANES] = rels[:, LANES:]
    kinds = (kinds_col[...] == lax.broadcasted_iota(jnp.int32, (edges, rel_count), 1)).astype(f32).astype(jnp.bfloat16)
    related = pick_rows(kinds, split_two(jnp.concatenate([rels[:, :LANES], wide_buf[:rel_count]], axis=1)))
    related = to_halves(related, width)
    slots_of = lambda s: (s, n - s) if s < mid else (s,)
    for s in range(1, mid + 1):
        for v in range(2):
            for d in range(2):
                u = v if d == 0 else 1 - v
                if ag_active(d, s, u):
                    slot = s if d == 0 else n - s
                    ag_copy(d, s, u).wait_recv()
                    if s < mid and ag_active(d, s + 1, u):
                        launch(ag_copy(d, s + 1, u))
                    if u == 1:
                        launch(cross_copy(slot))
                    launch(pair_copy(slot, u))
        if s > 1:
            for slot in slots_of(s - 1):
                relay(slot)
        if s > 2:
            for slot in slots_of(s - 2):
                gather(slot)
    for slot in slots_of(mid - 1):
        gather(slot)
    relay(mid)
    gather(mid)

    found = to_halves(rows[...], width)
    head, tail, contrast = found[:edges], found[edges : 2 * edges], found[2 * edges :]
    query = times(head, related)
    probe = times_conj(tail, related)
    positive = jnp.sum(query * tail, axis=1, keepdims=True)
    tail_loss, tail_struck, tail_back, tail_spread = one_side(query, positive, jnp.concatenate([tail, contrast], axis=0))
    head_loss, head_struck, head_back, head_spread = one_side(probe, positive, jnp.concatenate([head, contrast], axis=0))
    gain = tail_struck + head_struck - 2.0
    tail_back = tail_back + gain * tail
    grads = (
        times_conj(tail_back, related) + head_spread[:edges],
        gain * query + times(head_back, related) + tail_spread[:edges],
        tail_spread[edges:] + head_spread[edges:],
    )
    start = 0
    for part in grads:
        upper, lower = split_two(to_natural(part, width))
        grad_hi[start : start + part.shape[0]] = upper
        grad_lo[start : start + part.shape[0]] = lower
        start += part.shape[0]

    def sum_relations():
        rel_rows = to_natural(times_conj(tail_back, head) + times_conj(tail, head_back), width)
        kinds_t = (kinds_row[...] == lax.broadcasted_iota(jnp.int32, (rel_count, edges), 0)).astype(f32).astype(jnp.bfloat16)
        shape = rel_local.shape
        corner = (lax.rem(lax.broadcasted_iota(jnp.int32, shape, 0), rel_share) == 0) & (
            lax.broadcasted_iota(jnp.int32, shape, 1) == shape[1] - 1
        )
        rel_local[...] = pick_rows(kinds_t, split_two(rel_rows)) + jnp.where(corner, tail_loss + head_loss, 0.0)

    sum_relations()

    half = rs_sizes[0] + 2 * rs_sizes[1]
    mine = pl.multiple_of(core * half, 8)
    other = pl.multiple_of((1 - core) * half, 8)

    def half_copy(k):
        return send(pbuf.at[k, pl.ds(other, half)], dbuf.at[k], half_send.at[k], half_recv.at[k], partner)

    def over_copy(k):
        return send(pbuf.at[k, span(rs_sizes, core, 2)], abuf.at[k], over_send.at[k], over_recv.at[k], across)

    def contribute(k):
        owner = at(pos + k)
        onehot = (ids_row[...] - owner * shard == lax.broadcasted_iota(jnp.int32, (shard, reads), 0)).astype(f32).astype(jnp.bfloat16)
        total = pick_rows(onehot, (grad_hi[...], grad_lo[...]))
        pbuf[k, :shard] = total[:, :LANES]
        broad, thin = pack_extra(total[:, LANES:], width)
        pbuf[k, broad_at:thin_at] = broad
        pbuf[k, thin_at:packed] = thin
        share = rel_local[pl.ds(pl.multiple_of(owner * rel_share, 8), rel_share)]
        pbuf[k, packed : packed + rel_share] = share[:, :LANES]
        pbuf[k, packed + rel_share :] = share[:, LANES:]
        launch(half_copy(k))

    def pass_over(k):
        half_copy(k).wait_recv()
        pbuf[k, span(rs_sizes, core, 2)] += dbuf[k, span(rs_sizes, 0, 2)]
        launch(over_copy(k))

    def rs_active(d, s, u):
        return s > 1 or u == d

    def ring_rows(u):
        return pl.ds(0, rs_sizes[0]) if u == 0 else pl.ds(rs_sizes[0], rs_sizes[1])

    def rs_copy(d, s, u):
        k = (mid + 1 - s) if d == 0 else n - (mid + 1 - s)
        return send(
            pbuf.at[k, span(rs_sizes, core, u)],
            rbuf.at[d, s - 1, ring_rows(u)],
            rs_send.at[d, s - 1, u],
            rs_recv.at[d, s - 1, u],
            onward[d],
        )

    def ring_piece(d, s, u):
        k = (mid + 1 - s) if d == 0 else n - (mid + 1 - s)
        total = pbuf[k, span(rs_sizes, core, u)] + dbuf[k, span(rs_sizes, 0, u)]
        if u == 1:
            over_copy(k).wait_recv()
            total = total + abuf[k]
        if s > 1 and rs_active(d, s - 1, u):
            rs_copy(d, s - 1, u).wait_recv()
            total = total + rbuf[d, s - 2, ring_rows(u)]
        pbuf[k, span(rs_sizes, core, u)] = total
        launch(rs_copy(d, s, u))

    chunks_at = lambda s: (mid + 1 - s, n - (mid + 1 - s)) if s <= mid else (0,)
    contribute(mid)
    pass_over(mid)
    ring_piece(0, 1, 0)
    for k in chunks_at(2):
        contribute(k)
    ring_piece(1, 1, 1)
    for s in range(2, mid + 1):
        for k in chunks_at(s):
            pass_over(k)
        ahead = chunks_at(s + 1)
        for v in range(2):
            for d in range(2):
                ring_piece(d, s, (1 - d) if v == 0 else d)
            if v < len(ahead):
                contribute(ahead[v])
    pass_over(0)

    def last_copy(stage):
        if stage == 0:
            return send(fin, xbuf, last_send.at[0], last_recv.at[0], across)
        if stage == 1:
            where = full.at[span(rs_sizes, core, 1)]
            return send(where, where, last_send.at[1], last_recv.at[1], across)
        where = full.at[span(rs_sizes, core, stage - 2)]
        return send(where, where, last_send.at[stage], last_recv.at[stage], partner)

    for u in (1, 0):
        total = pbuf[0, span(rs_sizes, core, u)] + dbuf[0, span(rs_sizes, 0, u)]
        if u == 1:
            over_copy(0).wait_recv()
            total = total + abuf[0]
        for d in range(2):
            rs_copy(d, mid, u).wait_recv()
            total = total + rbuf[d, mid - 1, ring_rows(u)]
        if u == 1:
            full[span(rs_sizes, core, 1)] = total
            launch(last_copy(1))
            launch(last_copy(3))
        else:
            fin[...] = total
            launch(last_copy(0))
    last_copy(1).wait_recv()
    launch(last_copy(4))
    last_copy(0).wait_recv()
    full[span(rs_sizes, core, 0)] = fin[...] + xbuf[...]
    launch(last_copy(2))
    for stage in (3, 4, 2):
        last_copy(stage).wait_recv()

    def rel_copy(j):
        return send(full.at[pl.ds(packed, 2 * rel_share)], relbuf.at[j], rel_send.at[j], rel_recv.at[j], {"ea": lax.rem(me + j, n)})

    for j in range(1, n):
        launch(rel_copy(j))
    loss_out[...] = full[packed + rel_share : packed + rel_share + 8]
    extra = unpack_extra(full[broad_at:thin_at], full[thin_at:packed], width)
    base_step, extra_step, squares = update_of(full[:shard], extra, ent_hist[...], width)
    ent_out[:, :LANES] = base_step
    ent_out[:, LANES:] = extra_step[:, : width - LANES]
    ent_sq_out[...] = squares
    for j in range(n):
        if j:
            rel_copy(j).wait_recv()
            base, extra = relbuf[j, :rel_share], relbuf[j, rel_share:]
        else:
            base, extra = full[packed : packed + rel_share], full[packed + rel_share :]
        here = pl.ds(pl.multiple_of(lax.rem(me - j + n, n) * rel_share, 8), rel_share)
        base_step, extra_step, squares = update_of(base, extra, rel_hist[here], width)
        rel_out[here, :LANES] = base_step
        rel_out[here, LANES:] = extra_step[:, : width - LANES]
        rel_sq_out[here] = squares
    for copy in sent:
        copy.wait_send()


def piece_sizes(total, divisor):
    cross = total // divisor // 8 * 8
    return ((total - 4 * cross) // 2, cross)


def on_ring(entities, entity_history, relations, relation_history, edge_ends, edge_relations, negatives):
    n = lax.axis_size("ea")
    shard, width = entities.shape
    rel_count = relations.shape[0]
    edges = edge_ends.shape[0]
    ids = jnp.concatenate([edge_ends[:, 0], edge_ends[:, 1], negatives])
    reads = ids.shape[0]
    packed = shard * width // LANES
    chunk = packed + 2 * (rel_count // n)
    ag_sizes, rs_sizes = piece_sizes(packed, 6), piece_sizes(chunk, 7)
    half = chunk // 2
    wide = 2 * LANES
    mid = n // 2
    dma = pltpu.SemaphoreType.DMA
    vmem = pl.BlockSpec(memory_space=pltpu.VMEM)
    sems = [(2, mid, 2), (n, 3), (n,), (2, mid, 2), (n,), (n,), (5,), (n,)]
    entity_step, entity_squares, relation_step, relation_squares, loss = pl.pallas_call(
        functools.partial(step_kernel, n, ag_sizes, rs_sizes),
        out_shape=(
            jax.ShapeDtypeStruct((shard, width), f32),
            jax.ShapeDtypeStruct((shard, 1), f32),
            jax.ShapeDtypeStruct((rel_count, width), f32),
            jax.ShapeDtypeStruct((rel_count, 1), f32),
            jax.ShapeDtypeStruct((8, LANES), f32),
        ),
        in_specs=[vmem] * 8,
        out_specs=(vmem,) * 5,
        scratch_shapes=[
            pltpu.VMEM((n, packed, LANES), f32),
            pltpu.VMEM((max(shard, rel_count), LANES), f32),
            pltpu.VMEM((reads, wide), f32),
            pltpu.VMEM((reads, wide), jnp.bfloat16),
            pltpu.VMEM((reads, wide), jnp.bfloat16),
            pltpu.VMEM((rel_count, wide), f32),
            pltpu.VMEM((n, chunk, LANES), f32),
            pltpu.VMEM((n, half, LANES), f32),
            pltpu.VMEM((n, rs_sizes[1], LANES), f32),
            pltpu.VMEM((2, mid, sum(rs_sizes), LANES), f32),
            pltpu.VMEM((rs_sizes[0], LANES), f32),
            pltpu.VMEM((rs_sizes[0], LANES), f32),
            pltpu.VMEM((chunk, LANES), f32),
            pltpu.VMEM((n, 2 * (rel_count // n), LANES), f32),
        ]
        + [dma(shape) for shape in sems for both in range(2)],
        compiler_params=pltpu.CompilerParams(
            collective_id=0, has_side_effects=True, vmem_limit_bytes=60 * 1024 * 1024
        ),
    )(
        ids[:, None],
        ids[None, :],
        edge_relations[:, None],
        edge_relations[None, :],
        entities,
        entity_history[:, None],
        relations,
        relation_history[:, None],
    )
    mean_loss = (loss[0, LANES - 1] / (2.0 * edges * n * lax.axis_size("ba"))).reshape(1)
    return (entity_step, entity_squares[:, 0], relation_step, relation_squares[:, 0], mean_loss)


def fits_ring(n, n_ba, entities, relations):
    shard, width = entities.shape
    narrow = width - LANES - LANES // 2
    return (
        n_ba == 4
        and n % 2 == 0
        and 4 <= n <= 16
        and width % 2 == 0
        and 0 < narrow < LANES // 2 - 1
        and LANES % narrow == 0
        and shard % (8 * (LANES // narrow)) == 0
        and relations.shape[0] % (8 * n) == 0
    )


def per_device(entities, entity_history, relations, relation_history, *batch):
    fits = fits_ring(lax.axis_size("ea"), lax.axis_size("ba"), entities, relations)
    return (on_ring if fits else on_device)(entities, entity_history, relations, relation_history, *batch)


def solution(mesh):
    placed = (
        P("ea", None),
        P("ea"),
        P(),
        P(),
        P(("ba", "ea"), None),
        P(("ba", "ea")),
        P(("ba", "ea")),
    )
    return jax.shard_map(
        per_device,
        mesh=mesh,
        in_specs=placed,
        out_specs=(P("ea", None), P("ea"), P(), P(), P()),
        check_vma=False,
    )
```

```python
import functools

import jax
import jax.numpy as jnp
from jax import lax
from jax.experimental import pallas as pl
from jax.experimental.pallas import tpu as pltpu
from jax.sharding import PartitionSpec as P

learn_rate = 0.1
adagrad_eps = 1e-10
highest = lax.Precision.HIGHEST


def halves(vectors):
    half_width = vectors.shape[-1] // 2
    return (vectors[..., :half_width], vectors[..., half_width:])


def complex_times(former, latter):
    former_real, former_imag = halves(former)
    latter_real, latter_imag = halves(latter)
    return jnp.concatenate(
        [
            former_real * latter_real - former_imag * latter_imag,
            former_real * latter_imag + former_imag * latter_real,
        ],
        axis=-1,
    )


def conjugate(vectors):
    real_part, imag_part = halves(vectors)
    return jnp.concatenate([real_part, -imag_part], axis=-1)


def adagrad_step(slope_vector, history):
    squares = history + jnp.mean(slope_vector * slope_vector, axis=1)
    return (-learn_rate * slope_vector / (jnp.sqrt(squares)[:, None] + adagrad_eps), squares)


def bucket_slots(node_labels, shard_rows, peer_count, room_limit):
    owners = node_labels // shard_rows
    local_rows = node_labels - owners * shard_rows
    onehot = (owners[:, None] == jnp.arange(peer_count, dtype=jnp.int32)[None, :]).astype(jnp.int32)
    earlier = jnp.cumsum(onehot, axis=0) - onehot
    slot_positions = owners * room_limit + jnp.sum(earlier * onehot, axis=1)
    request = jnp.full((peer_count * room_limit,), -1, jnp.int32).at[slot_positions].set(local_rows)
    return (slot_positions, request.reshape(peer_count, room_limit))


def serve_rows(table, demanded_lookups):
    picked = jnp.take(table, jnp.maximum(demanded_lookups, 0), axis=0)
    return jnp.where((demanded_lookups >= 0)[..., None], picked, 0.0)


def outgoing_rows(slope_vector, slot_positions, peer_count, room_limit):
    buffer_rows = (
        jnp.zeros((peer_count * room_limit, slope_vector.shape[1]), jnp.float32)
        .at[slot_positions]
        .set(slope_vector)
    )
    return buffer_rows.reshape(peer_count, room_limit, slope_vector.shape[1])


def absorb(dense_grad, demanded_lookups, incoming):
    flat_rows = jnp.maximum(demanded_lookups, 0).reshape(-1)
    return dense_grad.at[flat_rows].add(incoming.reshape(-1, incoming.shape[-1]))


def matmul(former, latter):
    return jnp.dot(former, latter, precision=highest, preferred_element_type=jnp.float32)


def spread_back(weights, probe_rows):
    return lax.dot_general(
        weights,
        probe_rows,
        (((0,), (0,)), ((), ())),
        precision=highest,
        preferred_element_type=jnp.float32,
    )


def side_terms(probe_rows, positive, candidates):
    scores = lax.dot_general(
        probe_rows,
        candidates,
        (((1,), (1,)), ((), ())),
        precision=highest,
        preferred_element_type=jnp.float32,
    )
    own_edge = lax.broadcasted_iota(jnp.int32, scores.shape, 1) == lax.broadcasted_iota(
        jnp.int32, scores.shape, 0
    )
    scores = jnp.where(own_edge, -jnp.inf, scores)
    peak = jnp.maximum(jnp.max(scores, axis=1), positive)
    lifted = jnp.exp(scores - peak[:, None])
    struck = jnp.exp(positive - peak)
    normal = struck + jnp.sum(lifted, axis=1)
    loss_sum = jnp.sum(jnp.log(normal) + peak - positive)
    return (loss_sum, lifted / normal[:, None], struck / normal)


def on_device(
    entities, entity_history, relations, relation_history, edge_ends, edge_relations, negatives
):
    peer_count = lax.axis_size("ea")
    shard_rows = entities.shape[0]
    row_width = entities.shape[1]
    edge_count = edge_ends.shape[0]
    negative_count = negatives.shape[0]
    edge_share = edge_count // peer_count
    link_room = edge_share + max(1, edge_share // 2)
    negative_share = negative_count // peer_count
    contrast_room = negative_share + max(1, negative_share // 2)
    desired_items = (edge_ends[:, 0], edge_ends[:, 1], negatives)
    room_limits = (link_room, link_room, contrast_room)
    joint_capacity = sum(room_limits)
    joint_places, joint_request = bucket_slots(
        jnp.concatenate(desired_items), shard_rows, peer_count, joint_capacity
    )
    joint_asked = lax.all_to_all(joint_request, "ea", split_axis=0, concat_axis=0, tiled=True)
    joint_answer = lax.all_to_all(
        serve_rows(entities, joint_asked), "ea", split_axis=0, concat_axis=0, tiled=True
    )
    fetched = joint_answer.reshape(-1, row_width)[joint_places]
    head_rows = fetched[:edge_count]
    tail_rows = fetched[edge_count : 2 * edge_count]
    negative_rows = fetched[2 * edge_count :]
    related = jnp.take(relations, edge_relations, axis=0)
    tail_query = complex_times(head_rows, related)
    head_probe = complex_times(conjugate(related), tail_rows)
    positive = jnp.sum(tail_query * tail_rows, axis=1)
    tail_cands = jnp.concatenate([tail_rows, negative_rows], axis=0)
    head_cands = jnp.concatenate([head_rows, negative_rows], axis=0)
    tail_loss, tail_weight, tail_struck = side_terms(tail_query, positive, tail_cands)
    head_loss, head_weight, head_struck = side_terms(head_probe, positive, head_cands)
    gain = tail_struck + head_struck - 2.0
    tail_back = matmul(tail_weight, tail_cands) + gain[:, None] * tail_rows
    head_back = matmul(head_weight, head_cands)
    tail_spread = spread_back(tail_weight, tail_query)
    head_spread = spread_back(head_weight, head_probe)
    head_grad = complex_times(tail_back, conjugate(related)) + head_spread[:edge_count]
    tail_grad = (
        gain[:, None] * tail_query + complex_times(head_back, related) + tail_spread[:edge_count]
    )
    negative_grad = tail_spread[edge_count:] + head_spread[edge_count:]
    relation_rows = complex_times(tail_back, conjugate(head_rows)) + complex_times(
        conjugate(head_back), tail_rows
    )
    relation_local = jax.ops.segment_sum(
        relation_rows, edge_relations, num_segments=relations.shape[0]
    )
    loss_local = tail_loss + head_loss
    dense_grad = jnp.zeros((shard_rows, row_width), jnp.float32)
    joint_grad = jnp.concatenate([head_grad, tail_grad, negative_grad], axis=0)
    incoming = lax.all_to_all(
        outgoing_rows(joint_grad, joint_places, peer_count, joint_capacity),
        "ea",
        split_axis=0,
        concat_axis=0,
        tiled=True,
    )
    dense_grad = absorb(dense_grad, joint_asked, incoming)
    relation_sum, loss_sum = lax.psum((relation_local, loss_local), ("ea", "ba"))
    relation_step, relation_squares = adagrad_step(relation_sum, relation_history)
    mean_loss = (loss_sum / (2.0 * edge_count * peer_count * lax.axis_size("ba"))).reshape(1)
    summed = lax.psum(dense_grad, "ba")
    entity_step, entity_squares = adagrad_step(summed, entity_history)
    return (entity_step, entity_squares, relation_step, relation_squares, mean_loss)


LANES = 128
MESH = pl.DeviceIdType.MESH
f32 = jnp.float32


def split_two(values):
    upper = values.astype(jnp.bfloat16)
    return upper, (values - upper.astype(f32)).astype(jnp.bfloat16)


def dot_of(former, latter, dims):
    return lax.dot_general(former, latter, (dims, ((), ())), preferred_element_type=f32)


def dot_three(former, latter, dims):
    return dot_of(former[0], latter[0], dims) + (
        dot_of(former[0], latter[1], dims) + dot_of(former[1], latter[0], dims)
    )


def pick_rows(onehot, halves_of):
    dims = ((1,), (0,))
    return dot_of(onehot, halves_of[0], dims) + dot_of(onehot, halves_of[1], dims)


def times(former, latter):
    a, b = former[:, :LANES], former[:, LANES:]
    c, d = latter[:, :LANES], latter[:, LANES:]
    return jnp.concatenate([a * c - b * d, a * d + b * c], axis=1)


def times_conj(former, latter):
    a, b = former[:, :LANES], former[:, LANES:]
    c, d = latter[:, :LANES], latter[:, LANES:]
    return jnp.concatenate([a * c + b * d, b * c - a * d], axis=1)


def one_side(probe, positive, cands):
    probe_parts, cand_parts = split_two(probe), split_two(cands)
    scores = dot_three(probe_parts, cand_parts, ((1,), (1,)))
    own = lax.broadcasted_iota(jnp.int32, scores.shape, 1) == lax.broadcasted_iota(
        jnp.int32, scores.shape, 0
    )
    scores = jnp.where(own, -jnp.inf, scores)
    peak = jnp.maximum(jnp.max(scores, axis=1, keepdims=True), positive)
    lifted = jnp.exp(scores - peak)
    struck = jnp.exp(positive - peak)
    normal = struck + jnp.sum(lifted, axis=1, keepdims=True)
    loss = jnp.sum(jnp.log(normal) + peak - positive, axis=0, keepdims=True)
    weight = split_two(lifted / normal)
    back = dot_three(weight, cand_parts, ((1,), (0,)))
    spread = dot_three(weight, probe_parts, ((0,), (0,)))
    return loss, struck / normal, back, spread


def to_halves(turned, width):
    half = width // 2
    pad = jnp.zeros((LANES - half, turned.shape[1]), f32)
    return jnp.concatenate([turned[:half], pad, turned[half:width], pad], axis=0).T


def to_turned(halved, width):
    half = width // 2
    turned = halved.T
    return jnp.concatenate([turned[:half], turned[LANES : LANES + half]], axis=0)


def place_rows(turned, onehot):
    dims = ((1,), (1,))
    return dot_of(turned[0], onehot, dims) + dot_of(turned[1], onehot, dims)


def pick_turned(turned, onehot):
    dims = ((1,), (0,))
    return dot_of(turned[0], onehot, dims) + dot_of(turned[1], onehot, dims)


def update_of(total, history):
    squares = history + jnp.sum(total * total, axis=0, keepdims=True) / total.shape[0]
    return total * (-learn_rate / (jnp.sqrt(squares) + adagrad_eps)), squares


def step_kernel(
    n,
    ag_sizes,
    rs_sizes,
    ids_row,
    kinds_row,
    ent,
    ent_hist,
    rels,
    rel_hist,
    ent_out,
    ent_sq_out,
    rel_out,
    rel_sq_out,
    loss_out,
    tab,
    rows,
    grad_hi,
    grad_lo,
    rel_local,
    pbuf,
    dbuf,
    abuf,
    rbuf,
    fin,
    xbuf,
    full,
    relbuf,
    rel_sum,
    ag_send,
    ag_recv,
    pair_send,
    pair_recv,
    cross_send,
    cross_recv,
    rs_send,
    rs_recv,
    half_send,
    half_recv,
    over_send,
    over_recv,
    last_send,
    last_recv,
    rel_send,
    rel_recv,
):
    mid = n // 2
    width, shard = ent.shape
    rel_count = rels.shape[1]
    edges = kinds_row.shape[1]
    reads = ids_row.shape[1]
    rel_pad = rel_local.shape[0]
    rel_share = rel_pad // n
    side = shard // 2
    me = lax.axis_index("ea")
    lane = lax.axis_index("ba")
    core = lax.rem(lane, 2)
    plane = lane // 2

    def at(place):
        place = lax.rem(place + 2 * n, n)
        return 2 * place + (place // mid) * (2 * (n - place) - 1 - 2 * place)

    high, odd = me // 2, lax.rem(me, 2)
    pos = high + odd * (n - 1 - 2 * high)
    onward = ({"ea": at(pos + 1)}, {"ea": at(pos - 1)})
    partner = {"ba": lane + 1 - 2 * core}
    across = {"ba": lax.rem(lane + 2, 4)}

    barrier = pltpu.get_barrier_semaphore()
    for j in range(1, n):
        pl.semaphore_signal(barrier, inc=1, device_id={"ea": lax.rem(me + j, n)}, device_id_type=MESH)
    pl.semaphore_signal(barrier, inc=1, device_id=partner, device_id_type=MESH)
    pl.semaphore_signal(barrier, inc=1, device_id=across, device_id_type=MESH)

    pl.semaphore_wait(barrier, n + 1)

    sent = []

    def send(src, dst, send_sem, recv_sem, device):
        return pltpu.make_async_remote_copy(
            src_ref=src, dst_ref=dst, send_sem=send_sem, recv_sem=recv_sem,
            device_id=device, device_id_type=MESH,
        )

    def launch(copy):
        copy.start()
        sent.append(copy)

    def span(sizes, which_core, u):
        base, cross = sizes
        across_lanes = pl.ds(0, side) if which_core is None else pl.ds(pl.multiple_of(which_core * side, LANES), side)
        if u == 0:
            return pl.ds(0, base), across_lanes
        chosen = plane if u == 1 else 1 - plane
        return pl.ds(pl.multiple_of(base + chosen * cross, 8), cross), across_lanes

    def ag_active(d, s, u):
        return s < mid or (s == mid and u == d)

    def ag_copy(d, s, u):
        source = (s - 1) if d == 0 else (n - (s - 1)) % n
        target = s if d == 0 else n - s
        where = span(ag_sizes, core, u)
        src = ent.at[where] if s == 1 else tab.at[(source, *where)]
        return send(src, tab.at[(target, *where)], ag_send.at[d, s - 1, u], ag_recv.at[d, s - 1, u], onward[d])

    def pair_copy(slot, u):
        where = tab.at[(slot, *span(ag_sizes, core, u))]
        return send(where, where, pair_send.at[slot, u], pair_recv.at[slot, u], partner)

    def cross_copy(slot):
        where = tab.at[(slot, *span(ag_sizes, core, 1))]
        return send(where, where, cross_send.at[slot], cross_recv.at[slot], across)

    def relay(slot):
        cross_copy(slot).wait_recv()
        launch(pair_copy(slot, 2))

    def onehot_of(owner):
        places = lax.broadcasted_iota(jnp.int32, (shard, reads), 0)
        return (ids_row[...] - owner * shard == places).astype(f32).astype(jnp.bfloat16)

    def gather(slot):
        owner = at(pos - slot)
        onehot = onehot_of(owner)
        if slot:
            for u in range(3):
                pair_copy(slot, u).wait_recv()
        picked = pick_turned(split_two(tab[slot] if slot else ent[...]), onehot)
        if slot:
            rows[...] += picked
        else:
            rows[...] = picked

    for v in range(2):
        for d in range(2):
            launch(ag_copy(d, 1, v if d == 0 else 1 - v))
    gather(0)
    kinds = (kinds_row[...] == lax.broadcasted_iota(jnp.int32, (rel_count, edges), 0)).astype(f32).astype(jnp.bfloat16)
    related = to_halves(pick_turned(split_two(rels[...]), kinds), width)
    slots_of = lambda s: (s, n - s) if s < mid else (s,)
    for s in range(1, mid + 1):
        for v in range(2):
            for d in range(2):
                u = v if d == 0 else 1 - v
                if ag_active(d, s, u):
                    slot = s if d == 0 else n - s
                    ag_copy(d, s, u).wait_recv()
                    if s < mid and ag_active(d, s + 1, u):
                        launch(ag_copy(d, s + 1, u))
                    if u == 1:
                        launch(cross_copy(slot))
                    launch(pair_copy(slot, u))
        if s > 1:
            for slot in slots_of(s - 1):
                relay(slot)
        if s > 2:
            for slot in slots_of(s - 2):
                gather(slot)
    for slot in slots_of(mid - 1):
        gather(slot)
    relay(mid)
    gather(mid)

    found = to_halves(rows[...], width)
    head, tail, contrast = found[:edges], found[edges : 2 * edges], found[2 * edges :]
    query = times(head, related)
    probe = times_conj(tail, related)
    positive = jnp.sum(query * tail, axis=1, keepdims=True)
    tail_loss, tail_struck, tail_back, tail_spread = one_side(query, positive, jnp.concatenate([tail, contrast], axis=0))
    head_loss, head_struck, head_back, head_spread = one_side(probe, positive, jnp.concatenate([head, contrast], axis=0))
    gain = tail_struck + head_struck - 2.0
    tail_back = tail_back + gain * tail
    grads = (
        times_conj(tail_back, related) + head_spread[:edges],
        gain * query + times(head_back, related) + tail_spread[:edges],
        tail_spread[edges:] + head_spread[edges:],
    )
    start = 0
    for part in grads:
        upper, lower = split_two(to_turned(part, width))
        grad_hi[:, start : start + part.shape[0]] = upper
        grad_lo[:, start : start + part.shape[0]] = lower
        start += part.shape[0]
    rel_rows = to_turned(times_conj(tail_back, head) + times_conj(tail, head_back), width)
    rel_local[:width] = place_rows(split_two(rel_rows), kinds)
    corner = (rel_pad - width, rel_count)
    first = lax.broadcasted_iota(jnp.int32, corner, 0) + lax.broadcasted_iota(jnp.int32, corner, 1) == 0
    rel_local[width:] = jnp.where(first, tail_loss + head_loss, 0.0)

    other = pl.ds(pl.multiple_of((1 - core) * side, LANES), side)

    def half_copy(k):
        return send(pbuf.at[k, :, other], dbuf.at[k], half_send.at[k], half_recv.at[k], partner)

    def over_copy(k):
        return send(pbuf.at[(k, *span(rs_sizes, core, 2))], abuf.at[k], over_send.at[k], over_recv.at[k], across)

    def contribute(k):
        owner = at(pos + k)
        pbuf[k, :width] = place_rows((grad_hi[...], grad_lo[...]), onehot_of(owner))
        low = pl.multiple_of(owner * rel_share, 8)
        for part in range(2):
            share = rel_local[pl.ds(pl.multiple_of(low + part * (rel_share // 2), 8), rel_share // 2)]
            pbuf[k, width:, part * rel_count : (part + 1) * rel_count] = share
        launch(half_copy(k))

    def pass_over(k):
        half_copy(k).wait_recv()
        pbuf[(k, *span(rs_sizes, core, 2))] = pbuf[(k, *span(rs_sizes, core, 2))] + dbuf[(k, *span(rs_sizes, None, 2))]
        launch(over_copy(k))

    def rs_active(d, s, u):
        return s > 1 or u == d

    def ring_rows(u):
        return pl.ds(0, rs_sizes[0]) if u == 0 else pl.ds(rs_sizes[0], rs_sizes[1])

    def rs_copy(d, s, u):
        k = (mid + 1 - s) if d == 0 else n - (mid + 1 - s)
        return send(
            pbuf.at[(k, *span(rs_sizes, core, u))],
            rbuf.at[d, s - 1, ring_rows(u)],
            rs_send.at[d, s - 1, u],
            rs_recv.at[d, s - 1, u],
            onward[d],
        )

    def ring_piece(d, s, u):
        k = (mid + 1 - s) if d == 0 else n - (mid + 1 - s)
        total = pbuf[(k, *span(rs_sizes, core, u))] + dbuf[(k, *span(rs_sizes, None, u))]
        if u == 1:
            over_copy(k).wait_recv()
            total = total + abuf[k]
        if s > 1 and rs_active(d, s - 1, u):
            rs_copy(d, s - 1, u).wait_recv()
            total = total + rbuf[d, s - 2, ring_rows(u)]
        pbuf[(k, *span(rs_sizes, core, u))] = total
        launch(rs_copy(d, s, u))

    chunks_at = lambda s: (mid + 1 - s, n - (mid + 1 - s)) if s <= mid else (0,)
    contribute(mid)
    pass_over(mid)
    ring_piece(0, 1, 0)
    for k in chunks_at(2):
        contribute(k)
    ring_piece(1, 1, 1)
    for s in range(2, mid + 1):
        for k in chunks_at(s):
            pass_over(k)
        ahead = chunks_at(s + 1)
        for v in range(2):
            for d in range(2):
                ring_piece(d, s, (1 - d) if v == 0 else d)
            if v < len(ahead):
                contribute(ahead[v])
    pass_over(0)

    def last_copy(stage):
        if stage == 0:
            return send(fin, xbuf, last_send.at[0], last_recv.at[0], across)
        if stage == 1:
            where = full.at[span(rs_sizes, core, 1)]
            return send(where, where, last_send.at[1], last_recv.at[1], across)
        where = full.at[span(rs_sizes, core, stage - 2)]
        return send(where, where, last_send.at[stage], last_recv.at[stage], partner)

    for u in (1, 0):
        total = pbuf[(0, *span(rs_sizes, core, u))] + dbuf[(0, *span(rs_sizes, None, u))]
        if u == 1:
            over_copy(0).wait_recv()
            total = total + abuf[0]
        for d in range(2):
            rs_copy(d, mid, u).wait_recv()
            total = total + rbuf[d, mid - 1, ring_rows(u)]
        if u == 1:
            full[span(rs_sizes, core, 1)] = total
            launch(last_copy(1))
            launch(last_copy(3))
        else:
            fin[...] = total
            launch(last_copy(0))
    last_copy(1).wait_recv()
    launch(last_copy(4))
    last_copy(0).wait_recv()
    full[span(rs_sizes, core, 0)] = fin[...] + xbuf[...]
    launch(last_copy(2))
    for stage in (3, 4, 2):
        last_copy(stage).wait_recv()

    def rel_copy(j):
        return send(full.at[pl.ds(width, rel_share // 2)], relbuf.at[j], rel_send.at[j], rel_recv.at[j], {"ea": lax.rem(me + j, n)})

    for j in range(1, n):
        launch(rel_copy(j))
    ent_out[...], ent_sq_out[...] = update_of(full[:width], ent_hist[...])
    for j in range(n):
        if j:
            rel_copy(j).wait_recv()
        low = pl.multiple_of(lax.rem(me - j + n, n) * rel_share, 8)
        for part in range(2):
            columns = pl.ds(part * rel_count, rel_count)
            share = relbuf[j, :, columns] if j else full[pl.ds(width, rel_share // 2), columns]
            rel_sum[pl.ds(pl.multiple_of(low + part * (rel_share // 2), 8), rel_share // 2)] = share
    rel_out[...], rel_sq_out[...] = update_of(rel_sum[:width], rel_hist[...])
    loss_out[...] = rel_sum[width : width + 8, :LANES]
    for copy in sent:
        copy.wait_send()


def piece_sizes(total, divisor):
    cross = total // divisor // 8 * 8
    return (total - 2 * cross, cross)


def on_ring(entities, entity_history, relations, relation_history, edge_ends, edge_relations, negatives):
    n = lax.axis_size("ea")
    shard, width = entities.shape
    rel_count = relations.shape[0]
    edges = edge_ends.shape[0]
    ids = jnp.concatenate([edge_ends[:, 0], edge_ends[:, 1], negatives])
    reads = ids.shape[0]
    rel_pad = -(-(width + 8) // (16 * n)) * 16 * n
    chunk = width + rel_pad // n // 2
    ag_sizes, rs_sizes = piece_sizes(width, 3), piece_sizes(chunk, 3)
    side = shard // 2
    mid = n // 2
    dma = pltpu.SemaphoreType.DMA
    vmem = pl.BlockSpec(memory_space=pltpu.VMEM)
    sems = [(2, mid, 2), (n, 3), (n,), (2, mid, 2), (n,), (n,), (5,), (n,)]
    entity_step, entity_squares, relation_step, relation_squares, loss = pl.pallas_call(
        functools.partial(step_kernel, n, ag_sizes, rs_sizes),
        out_shape=(
            jax.ShapeDtypeStruct((width, shard), f32),
            jax.ShapeDtypeStruct((1, shard), f32),
            jax.ShapeDtypeStruct((width, rel_count), f32),
            jax.ShapeDtypeStruct((1, rel_count), f32),
            jax.ShapeDtypeStruct((8, LANES), f32),
        ),
        in_specs=[vmem] * 6,
        out_specs=(vmem,) * 5,
        scratch_shapes=[
            pltpu.VMEM((n, width, shard), f32),
            pltpu.VMEM((width, reads), f32),
            pltpu.VMEM((width, reads), jnp.bfloat16),
            pltpu.VMEM((width, reads), jnp.bfloat16),
            pltpu.VMEM((rel_pad, rel_count), f32),
            pltpu.VMEM((n, chunk, shard), f32),
            pltpu.VMEM((n, chunk, side), f32),
            pltpu.VMEM((n, rs_sizes[1], side), f32),
            pltpu.VMEM((2, mid, sum(rs_sizes), side), f32),
            pltpu.VMEM((rs_sizes[0], side), f32),
            pltpu.VMEM((rs_sizes[0], side), f32),
            pltpu.VMEM((chunk, shard), f32),
            pltpu.VMEM((n, rel_pad // n // 2, shard), f32),
            pltpu.VMEM((rel_pad, rel_count), f32),
        ]
        + [dma(shape) for shape in sems for both in range(2)],
        compiler_params=pltpu.CompilerParams(
            collective_id=0, has_side_effects=True, vmem_limit_bytes=60 * 1024 * 1024
        ),
    )(
        ids[None, :],
        edge_relations[None, :],
        entities.T,
        entity_history[None, :],
        relations.T,
        relation_history[None, :],
    )
    mean_loss = (loss[0, 0] / (2.0 * edges * n * lax.axis_size("ba"))).reshape(1)
    return (entity_step.T, entity_squares[0], relation_step.T, relation_squares[0], mean_loss)


def fits_ring(n, n_ba, entities, relations):
    shard, width = entities.shape
    return (
        n_ba == 4
        and n % 2 == 0
        and 4 <= n <= 16
        and width % 8 == 0
        and width <= 2 * LANES
        and shard % (2 * LANES) == 0
        and 2 * relations.shape[0] == shard
    )


def per_device(entities, entity_history, relations, relation_history, *batch):
    fits = fits_ring(lax.axis_size("ea"), lax.axis_size("ba"), entities, relations)
    return (on_ring if fits else on_device)(entities, entity_history, relations, relation_history, *batch)


def solution(mesh):
    placed = (
        P("ea", None),
        P("ea"),
        P(),
        P(),
        P(("ba", "ea"), None),
        P(("ba", "ea")),
        P(("ba", "ea")),
    )
    return jax.shard_map(
        per_device,
        mesh=mesh,
        in_specs=placed,
        out_specs=(P("ea", None), P("ea"), P(), P(), P()),
        check_vma=False,
    )
```

```python
import functools

import jax
import jax.numpy as jnp
from jax import lax
from jax.experimental import pallas as pl
from jax.experimental.pallas import tpu as pltpu
from jax.sharding import PartitionSpec as P

learn_rate = 0.1
adagrad_eps = 1e-10
highest = lax.Precision.HIGHEST


def halves(vectors):
    half_width = vectors.shape[-1] // 2
    return (vectors[..., :half_width], vectors[..., half_width:])


def complex_times(former, latter):
    former_real, former_imag = halves(former)
    latter_real, latter_imag = halves(latter)
    return jnp.concatenate(
        [
            former_real * latter_real - former_imag * latter_imag,
            former_real * latter_imag + former_imag * latter_real,
        ],
        axis=-1,
    )


def conjugate(vectors):
    real_part, imag_part = halves(vectors)
    return jnp.concatenate([real_part, -imag_part], axis=-1)


def adagrad_step(slope_vector, history):
    squares = history + jnp.mean(slope_vector * slope_vector, axis=1)
    return (-learn_rate * slope_vector / (jnp.sqrt(squares)[:, None] + adagrad_eps), squares)


def bucket_slots(node_labels, shard_rows, peer_count, room_limit):
    owners = node_labels // shard_rows
    local_rows = node_labels - owners * shard_rows
    onehot = (owners[:, None] == jnp.arange(peer_count, dtype=jnp.int32)[None, :]).astype(jnp.int32)
    earlier = jnp.cumsum(onehot, axis=0) - onehot
    slot_positions = owners * room_limit + jnp.sum(earlier * onehot, axis=1)
    request = jnp.full((peer_count * room_limit,), -1, jnp.int32).at[slot_positions].set(local_rows)
    return (slot_positions, request.reshape(peer_count, room_limit))


def serve_rows(table, demanded_lookups):
    picked = jnp.take(table, jnp.maximum(demanded_lookups, 0), axis=0)
    return jnp.where((demanded_lookups >= 0)[..., None], picked, 0.0)


def outgoing_rows(slope_vector, slot_positions, peer_count, room_limit):
    buffer_rows = (
        jnp.zeros((peer_count * room_limit, slope_vector.shape[1]), jnp.float32)
        .at[slot_positions]
        .set(slope_vector)
    )
    return buffer_rows.reshape(peer_count, room_limit, slope_vector.shape[1])


def absorb(dense_grad, demanded_lookups, incoming):
    flat_rows = jnp.maximum(demanded_lookups, 0).reshape(-1)
    return dense_grad.at[flat_rows].add(incoming.reshape(-1, incoming.shape[-1]))


def matmul(former, latter):
    return jnp.dot(former, latter, precision=highest, preferred_element_type=jnp.float32)


def spread_back(weights, probe_rows):
    return lax.dot_general(
        weights,
        probe_rows,
        (((0,), (0,)), ((), ())),
        precision=highest,
        preferred_element_type=jnp.float32,
    )


def side_terms(probe_rows, positive, candidates):
    scores = lax.dot_general(
        probe_rows,
        candidates,
        (((1,), (1,)), ((), ())),
        precision=highest,
        preferred_element_type=jnp.float32,
    )
    own_edge = lax.broadcasted_iota(jnp.int32, scores.shape, 1) == lax.broadcasted_iota(
        jnp.int32, scores.shape, 0
    )
    scores = jnp.where(own_edge, -jnp.inf, scores)
    peak = jnp.maximum(jnp.max(scores, axis=1), positive)
    lifted = jnp.exp(scores - peak[:, None])
    struck = jnp.exp(positive - peak)
    normal = struck + jnp.sum(lifted, axis=1)
    loss_sum = jnp.sum(jnp.log(normal) + peak - positive)
    return (loss_sum, lifted / normal[:, None], struck / normal)


def on_device(
    entities, entity_history, relations, relation_history, edge_ends, edge_relations, negatives
):
    peer_count = lax.axis_size("ea")
    shard_rows = entities.shape[0]
    row_width = entities.shape[1]
    edge_count = edge_ends.shape[0]
    negative_count = negatives.shape[0]
    edge_share = edge_count // peer_count
    link_room = edge_share + max(1, edge_share // 2)
    negative_share = negative_count // peer_count
    contrast_room = negative_share + max(1, negative_share // 2)
    desired_items = (edge_ends[:, 0], edge_ends[:, 1], negatives)
    room_limits = (link_room, link_room, contrast_room)
    joint_capacity = sum(room_limits)
    joint_places, joint_request = bucket_slots(
        jnp.concatenate(desired_items), shard_rows, peer_count, joint_capacity
    )
    joint_asked = lax.all_to_all(joint_request, "ea", split_axis=0, concat_axis=0, tiled=True)
    joint_answer = lax.all_to_all(
        serve_rows(entities, joint_asked), "ea", split_axis=0, concat_axis=0, tiled=True
    )
    fetched = joint_answer.reshape(-1, row_width)[joint_places]
    head_rows = fetched[:edge_count]
    tail_rows = fetched[edge_count : 2 * edge_count]
    negative_rows = fetched[2 * edge_count :]
    related = jnp.take(relations, edge_relations, axis=0)
    tail_query = complex_times(head_rows, related)
    head_probe = complex_times(conjugate(related), tail_rows)
    positive = jnp.sum(tail_query * tail_rows, axis=1)
    tail_cands = jnp.concatenate([tail_rows, negative_rows], axis=0)
    head_cands = jnp.concatenate([head_rows, negative_rows], axis=0)
    tail_loss, tail_weight, tail_struck = side_terms(tail_query, positive, tail_cands)
    head_loss, head_weight, head_struck = side_terms(head_probe, positive, head_cands)
    gain = tail_struck + head_struck - 2.0
    tail_back = matmul(tail_weight, tail_cands) + gain[:, None] * tail_rows
    head_back = matmul(head_weight, head_cands)
    tail_spread = spread_back(tail_weight, tail_query)
    head_spread = spread_back(head_weight, head_probe)
    head_grad = complex_times(tail_back, conjugate(related)) + head_spread[:edge_count]
    tail_grad = (
        gain[:, None] * tail_query + complex_times(head_back, related) + tail_spread[:edge_count]
    )
    negative_grad = tail_spread[edge_count:] + head_spread[edge_count:]
    relation_rows = complex_times(tail_back, conjugate(head_rows)) + complex_times(
        conjugate(head_back), tail_rows
    )
    relation_local = jax.ops.segment_sum(
        relation_rows, edge_relations, num_segments=relations.shape[0]
    )
    loss_local = tail_loss + head_loss
    dense_grad = jnp.zeros((shard_rows, row_width), jnp.float32)
    joint_grad = jnp.concatenate([head_grad, tail_grad, negative_grad], axis=0)
    incoming = lax.all_to_all(
        outgoing_rows(joint_grad, joint_places, peer_count, joint_capacity),
        "ea",
        split_axis=0,
        concat_axis=0,
        tiled=True,
    )
    dense_grad = absorb(dense_grad, joint_asked, incoming)
    relation_sum, loss_sum = lax.psum((relation_local, loss_local), ("ea", "ba"))
    relation_step, relation_squares = adagrad_step(relation_sum, relation_history)
    mean_loss = (loss_sum / (2.0 * edge_count * peer_count * lax.axis_size("ba"))).reshape(1)
    summed = lax.psum(dense_grad, "ba")
    entity_step, entity_squares = adagrad_step(summed, entity_history)
    return (entity_step, entity_squares, relation_step, relation_squares, mean_loss)


LANES = 128
MESH = pl.DeviceIdType.MESH
f32 = jnp.float32


def split_two(values):
    upper = values.astype(jnp.bfloat16)
    return upper, (values - upper.astype(f32)).astype(jnp.bfloat16)


def dot_of(former, latter, dims):
    return lax.dot_general(former, latter, (dims, ((), ())), preferred_element_type=f32)


def dot_three(former, latter, dims):
    return dot_of(former[0], latter[0], dims) + (
        dot_of(former[0], latter[1], dims) + dot_of(former[1], latter[0], dims)
    )


def pick_rows(onehot, halves_of):
    dims = ((1,), (0,))
    return dot_of(onehot, halves_of[0], dims) + dot_of(onehot, halves_of[1], dims)


def times(former, latter):
    a, b = former[:, :LANES], former[:, LANES:]
    c, d = latter[:, :LANES], latter[:, LANES:]
    return jnp.concatenate([a * c - b * d, a * d + b * c], axis=1)


def times_conj(former, latter):
    a, b = former[:, :LANES], former[:, LANES:]
    c, d = latter[:, :LANES], latter[:, LANES:]
    return jnp.concatenate([a * c + b * d, b * c - a * d], axis=1)


def one_side(probe, positive, cands):
    probe_parts, cand_parts = split_two(probe), split_two(cands)
    scores = dot_three(probe_parts, cand_parts, ((1,), (1,)))
    own = lax.broadcasted_iota(jnp.int32, scores.shape, 1) == lax.broadcasted_iota(
        jnp.int32, scores.shape, 0
    )
    scores = jnp.where(own, -jnp.inf, scores)
    peak = jnp.maximum(jnp.max(scores, axis=1, keepdims=True), positive)
    lifted = jnp.exp(scores - peak)
    struck = jnp.exp(positive - peak)
    normal = struck + jnp.sum(lifted, axis=1, keepdims=True)
    loss = jnp.sum(jnp.log(normal) + peak - positive, axis=0, keepdims=True)
    weight = split_two(lifted / normal)
    back = dot_three(weight, cand_parts, ((1,), (0,)))
    spread = dot_three(weight, probe_parts, ((0,), (0,)))
    return loss, struck / normal, back, spread


def to_halves(turned, width):
    half = width // 2
    pad = jnp.zeros((LANES - half, turned.shape[1]), f32)
    return jnp.concatenate([turned[:half], pad, turned[half:width], pad], axis=0).T


def to_turned(halved, width):
    half = width // 2
    turned = halved.T
    return jnp.concatenate([turned[:half], turned[LANES : LANES + half]], axis=0)


def place_rows(turned, onehot):
    dims = ((1,), (1,))
    return dot_of(turned[0], onehot, dims) + dot_of(turned[1], onehot, dims)


def pick_turned(turned, onehot):
    dims = ((1,), (0,))
    return dot_of(turned[0], onehot, dims) + dot_of(turned[1], onehot, dims)


def update_of(total, history):
    squares = history + jnp.sum(total * total, axis=0, keepdims=True) / total.shape[0]
    return total * (-learn_rate / (jnp.sqrt(squares) + adagrad_eps)), squares


def step_kernel(
    n,
    ag_sizes,
    rs_sizes,
    ids_row,
    kinds_row,
    ent,
    ent_hist,
    rels,
    rel_hist,
    ent_out,
    ent_sq_out,
    rel_out,
    rel_sq_out,
    loss_out,
    tab,
    rows,
    grad_hi,
    grad_lo,
    rel_local,
    pbuf,
    dbuf,
    abuf,
    rbuf,
    fin,
    xbuf,
    full,
    relbuf,
    rel_sum,
    ag_send,
    ag_recv,
    pair_send,
    pair_recv,
    cross_send,
    cross_recv,
    rs_send,
    rs_recv,
    half_send,
    half_recv,
    over_send,
    over_recv,
    last_send,
    last_recv,
    rel_send,
    rel_recv,
):
    mid = n // 2
    width, shard = ent.shape
    rel_count = rels.shape[1]
    edges = kinds_row.shape[1]
    reads = ids_row.shape[1]
    rel_pad = rel_local.shape[0]
    rel_share = rel_pad // n
    side = shard // 2
    me = lax.axis_index("ea")
    lane = lax.axis_index("ba")
    core = lax.rem(lane, 2)
    plane = lane // 2

    def at(place):
        place = lax.rem(place + 2 * n, n)
        return 2 * place + (place // mid) * (2 * (n - place) - 1 - 2 * place)

    high, odd = me // 2, lax.rem(me, 2)
    pos = high + odd * (n - 1 - 2 * high)
    onward = ({"ea": at(pos + 1)}, {"ea": at(pos - 1)})
    partner = {"ba": lane + 1 - 2 * core}
    across = {"ba": lax.rem(lane + 2, 4)}

    barrier = pltpu.get_barrier_semaphore()
    for j in range(1, n):
        pl.semaphore_signal(barrier, inc=1, device_id={"ea": lax.rem(me + j, n)}, device_id_type=MESH)
    pl.semaphore_signal(barrier, inc=1, device_id=partner, device_id_type=MESH)
    pl.semaphore_signal(barrier, inc=1, device_id=across, device_id_type=MESH)

    pl.semaphore_wait(barrier, n + 1)

    sent = []

    def send(src, dst, send_sem, recv_sem, device):
        return pltpu.make_async_remote_copy(
            src_ref=src, dst_ref=dst, send_sem=send_sem, recv_sem=recv_sem,
            device_id=device, device_id_type=MESH,
        )

    def launch(copy):
        copy.start()
        sent.append(copy)

    def span(sizes, which_core, u):
        base, cross = sizes
        across_lanes = pl.ds(0, side) if which_core is None else pl.ds(pl.multiple_of(which_core * side, LANES), side)
        if u == 0:
            return pl.ds(0, base), across_lanes
        chosen = plane if u == 1 else 1 - plane
        return pl.ds(pl.multiple_of(base + chosen * cross, 8), cross), across_lanes

    def ag_active(d, s, u):
        return s < mid or (s == mid and u == d)

    def ag_copy(d, s, u):
        source = (s - 1) if d == 0 else (n - (s - 1)) % n
        target = s if d == 0 else n - s
        where = span(ag_sizes, core, u)
        src = ent.at[where] if s == 1 else tab.at[(source, *where)]
        return send(src, tab.at[(target, *where)], ag_send.at[d, s - 1, u], ag_recv.at[d, s - 1, u], onward[d])

    def pair_copy(slot, u):
        where = tab.at[(slot, *span(ag_sizes, core, u))]
        return send(where, where, pair_send.at[slot, u], pair_recv.at[slot, u], partner)

    def cross_copy(slot):
        where = tab.at[(slot, *span(ag_sizes, core, 1))]
        return send(where, where, cross_send.at[slot], cross_recv.at[slot], across)

    def relay(slot):
        cross_copy(slot).wait_recv()
        launch(pair_copy(slot, 2))

    def onehot_of(owner):
        places = lax.broadcasted_iota(jnp.int32, (shard, reads), 0)
        return (ids_row[...] - owner * shard == places).astype(f32).astype(jnp.bfloat16)

    def gather(slot):
        owner = at(pos - slot)
        onehot = onehot_of(owner)
        if slot:
            for u in range(3):
                pair_copy(slot, u).wait_recv()
        picked = pick_turned(split_two(tab[slot] if slot else ent[...]), onehot)
        if slot:
            rows[...] += picked
        else:
            rows[...] = picked

    for v in range(2):
        for d in range(2):
            launch(ag_copy(d, 1, v if d == 0 else 1 - v))
    gather(0)
    kinds = (kinds_row[...] == lax.broadcasted_iota(jnp.int32, (rel_count, edges), 0)).astype(f32).astype(jnp.bfloat16)
    related = to_halves(pick_turned(split_two(rels[...]), kinds), width)
    slots_of = lambda s: (s, n - s) if s < mid else (s,)
    for s in range(1, mid + 1):
        for v in range(2):
            for d in range(2):
                u = v if d == 0 else 1 - v
                if ag_active(d, s, u):
                    slot = s if d == 0 else n - s
                    ag_copy(d, s, u).wait_recv()
                    if s < mid and ag_active(d, s + 1, u):
                        launch(ag_copy(d, s + 1, u))
                    if u == 1:
                        launch(cross_copy(slot))
                    launch(pair_copy(slot, u))
        if s > 1:
            for slot in slots_of(s - 1):
                relay(slot)
        if s > 2:
            for slot in slots_of(s - 2):
                gather(slot)
    for slot in slots_of(mid - 1):
        gather(slot)
    relay(mid)
    gather(mid)

    found = to_halves(rows[...], width)
    head, tail, contrast = found[:edges], found[edges : 2 * edges], found[2 * edges :]
    query = times(head, related)
    probe = times_conj(tail, related)
    positive = jnp.sum(query * tail, axis=1, keepdims=True)
    tail_loss, tail_struck, tail_back, tail_spread = one_side(query, positive, jnp.concatenate([tail, contrast], axis=0))
    head_loss, head_struck, head_back, head_spread = one_side(probe, positive, jnp.concatenate([head, contrast], axis=0))
    gain = tail_struck + head_struck - 2.0
    tail_back = tail_back + gain * tail
    grads = (
        times_conj(tail_back, related) + head_spread[:edges],
        gain * query + times(head_back, related) + tail_spread[:edges],
        tail_spread[edges:] + head_spread[edges:],
    )
    start = 0
    for part in grads:
        upper, lower = split_two(to_turned(part, width))
        grad_hi[:, start : start + part.shape[0]] = upper
        grad_lo[:, start : start + part.shape[0]] = lower
        start += part.shape[0]
    rel_rows = to_turned(times_conj(tail_back, head) + times_conj(tail, head_back), width)
    rel_local[:width] = place_rows(split_two(rel_rows), kinds)
    corner = (rel_pad - width, rel_count)
    first = lax.broadcasted_iota(jnp.int32, corner, 0) + lax.broadcasted_iota(jnp.int32, corner, 1) == 0
    rel_local[width:] = jnp.where(first, tail_loss + head_loss, 0.0)

    other = pl.ds(pl.multiple_of((1 - core) * side, LANES), side)

    def half_copy(k):
        return send(pbuf.at[k, :, other], dbuf.at[k], half_send.at[k], half_recv.at[k], partner)

    def over_copy(k):
        return send(pbuf.at[(k, *span(rs_sizes, core, 2))], abuf.at[k], over_send.at[k], over_recv.at[k], across)

    def contribute(k):
        owner = at(pos + k)
        pbuf[k, :width] = place_rows((grad_hi[...], grad_lo[...]), onehot_of(owner))
        low = pl.multiple_of(owner * rel_share, 8)
        for part in range(2):
            share = rel_local[pl.ds(pl.multiple_of(low + part * (rel_share // 2), 8), rel_share // 2)]
            pbuf[k, width:, part * rel_count : (part + 1) * rel_count] = share
        launch(half_copy(k))

    def pass_over(k):
        half_copy(k).wait_recv()
        pbuf[(k, *span(rs_sizes, core, 2))] = pbuf[(k, *span(rs_sizes, core, 2))] + dbuf[(k, *span(rs_sizes, None, 2))]
        launch(over_copy(k))

    def rs_active(d, s, u):
        return s > 1 or u == d

    def ring_rows(u):
        return pl.ds(0, rs_sizes[0]) if u == 0 else pl.ds(rs_sizes[0], rs_sizes[1])

    def rs_copy(d, s, u):
        k = (mid + 1 - s) if d == 0 else n - (mid + 1 - s)
        return send(
            pbuf.at[(k, *span(rs_sizes, core, u))],
            rbuf.at[d, s - 1, ring_rows(u)],
            rs_send.at[d, s - 1, u],
            rs_recv.at[d, s - 1, u],
            onward[d],
        )

    def ring_piece(d, s, u):
        k = (mid + 1 - s) if d == 0 else n - (mid + 1 - s)
        total = pbuf[(k, *span(rs_sizes, core, u))] + dbuf[(k, *span(rs_sizes, None, u))]
        if u == 1:
            over_copy(k).wait_recv()
            total = total + abuf[k]
        if s > 1 and rs_active(d, s - 1, u):
            rs_copy(d, s - 1, u).wait_recv()
            total = total + rbuf[d, s - 2, ring_rows(u)]
        pbuf[(k, *span(rs_sizes, core, u))] = total
        launch(rs_copy(d, s, u))

    chunks_at = lambda s: (mid + 1 - s, n - (mid + 1 - s)) if s <= mid else (0,)
    contribute(mid)
    pass_over(mid)
    ring_piece(0, 1, 0)
    for k in chunks_at(2):
        contribute(k)
    ring_piece(1, 1, 1)
    for s in range(2, mid + 1):
        for k in chunks_at(s):
            pass_over(k)
        ahead = chunks_at(s + 1)
        for v in range(2):
            for d in range(2):
                ring_piece(d, s, (1 - d) if v == 0 else d)
            if v < len(ahead):
                contribute(ahead[v])
    pass_over(0)

    def last_copy(stage):
        if stage == 0:
            return send(fin, xbuf, last_send.at[0], last_recv.at[0], across)
        if stage == 1:
            where = full.at[span(rs_sizes, core, 1)]
            return send(where, where, last_send.at[1], last_recv.at[1], across)
        where = full.at[span(rs_sizes, core, stage - 2)]
        return send(where, where, last_send.at[stage], last_recv.at[stage], partner)

    for u in (1, 0):
        total = pbuf[(0, *span(rs_sizes, core, u))] + dbuf[(0, *span(rs_sizes, None, u))]
        if u == 1:
            over_copy(0).wait_recv()
            total = total + abuf[0]
        for d in range(2):
            rs_copy(d, mid, u).wait_recv()
            total = total + rbuf[d, mid - 1, ring_rows(u)]
        if u == 1:
            full[span(rs_sizes, core, 1)] = total
            launch(last_copy(1))
            launch(last_copy(3))
        else:
            fin[...] = total
            launch(last_copy(0))
    last_copy(1).wait_recv()
    launch(last_copy(4))
    for stage in (3, 4):
        last_copy(stage).wait_recv()

    def rel_copy(j):
        return send(full.at[pl.ds(width, rel_share // 2)], relbuf.at[j], rel_send.at[j], rel_recv.at[j], {"ea": lax.rem(me + j, n)})

    for j in range(1, n):
        launch(rel_copy(j))
    last_copy(0).wait_recv()
    full[span(rs_sizes, core, 0)] = fin[...] + xbuf[...]
    launch(last_copy(2))
    last_copy(2).wait_recv()

    ent_out[...], ent_sq_out[...] = update_of(full[:width], ent_hist[...])
    for j in range(n):
        if j:
            rel_copy(j).wait_recv()
        low = pl.multiple_of(lax.rem(me - j + n, n) * rel_share, 8)
        for part in range(2):
            columns = pl.ds(part * rel_count, rel_count)
            share = relbuf[j, :, columns] if j else full[pl.ds(width, rel_share // 2), columns]
            rel_sum[pl.ds(pl.multiple_of(low + part * (rel_share // 2), 8), rel_share // 2)] = share
    rel_out[...], rel_sq_out[...] = update_of(rel_sum[:width], rel_hist[...])
    loss_out[...] = rel_sum[width : width + 1, :1] / (2.0 * edges * n * 4)
    for copy in sent:
        copy.wait_send()


def piece_sizes(total, divisor):
    cross = total // divisor // 8 * 8
    return (total - 2 * cross, cross)


def on_ring(entities, entity_history, relations, relation_history, edge_ends, edge_relations, negatives):
    n = lax.axis_size("ea")
    shard, width = entities.shape
    rel_count = relations.shape[0]
    edges = edge_ends.shape[0]
    ids = jnp.concatenate([edge_ends[:, 0], edge_ends[:, 1], negatives])
    reads = ids.shape[0]
    rel_pad = -(-(width + 8) // (16 * n)) * 16 * n
    chunk = width + rel_pad // n // 2
    ag_sizes, rs_sizes = piece_sizes(width, 3), piece_sizes(chunk, 3)
    side = shard // 2
    mid = n // 2
    dma = pltpu.SemaphoreType.DMA
    vmem = pl.BlockSpec(memory_space=pltpu.VMEM)
    sems = [(2, mid, 2), (n, 3), (n,), (2, mid, 2), (n,), (n,), (5,), (n,)]
    entity_step, entity_squares, relation_step, relation_squares, loss = pl.pallas_call(
        functools.partial(step_kernel, n, ag_sizes, rs_sizes),
        out_shape=(
            jax.ShapeDtypeStruct((width, shard), f32),
            jax.ShapeDtypeStruct((1, shard), f32),
            jax.ShapeDtypeStruct((width, rel_count), f32),
            jax.ShapeDtypeStruct((1, rel_count), f32),
            jax.ShapeDtypeStruct((1, 1), f32),
        ),
        in_specs=[vmem] * 6,
        out_specs=(vmem,) * 5,
        scratch_shapes=[
            pltpu.VMEM((n, width, shard), f32),
            pltpu.VMEM((width, reads), f32),
            pltpu.VMEM((width, reads), jnp.bfloat16),
            pltpu.VMEM((width, reads), jnp.bfloat16),
            pltpu.VMEM((rel_pad, rel_count), f32),
            pltpu.VMEM((n, chunk, shard), f32),
            pltpu.VMEM((n, chunk, side), f32),
            pltpu.VMEM((n, rs_sizes[1], side), f32),
            pltpu.VMEM((2, mid, sum(rs_sizes), side), f32),
            pltpu.VMEM((rs_sizes[0], side), f32),
            pltpu.VMEM((rs_sizes[0], side), f32),
            pltpu.VMEM((chunk, shard), f32),
            pltpu.VMEM((n, rel_pad // n // 2, shard), f32),
            pltpu.VMEM((rel_pad, rel_count), f32),
        ]
        + [dma(shape) for shape in sems for both in range(2)],
        compiler_params=pltpu.CompilerParams(
            collective_id=0, has_side_effects=True, vmem_limit_bytes=60 * 1024 * 1024
        ),
    )(
        ids[None, :],
        edge_relations[None, :],
        entities.T,
        entity_history[None, :],
        relations.T,
        relation_history[None, :],
    )
    mean_loss = loss.reshape(1)
    return (entity_step.T, entity_squares[0], relation_step.T, relation_squares[0], mean_loss)


def fits_ring(n, n_ba, entities, relations):
    shard, width = entities.shape
    return (
        n_ba == 4
        and n % 2 == 0
        and 4 <= n <= 16
        and width % 8 == 0
        and width <= 2 * LANES
        and shard % (2 * LANES) == 0
        and 2 * relations.shape[0] == shard
        and 3 * (width // 8) > 2 * n
    )


def per_device(entities, entity_history, relations, relation_history, *batch):
    fits = fits_ring(lax.axis_size("ea"), lax.axis_size("ba"), entities, relations)
    return (on_ring if fits else on_device)(entities, entity_history, relations, relation_history, *batch)


def solution(mesh):
    placed = (
        P("ea", None),
        P("ea"),
        P(),
        P(),
        P(("ba", "ea"), None),
        P(("ba", "ea")),
        P(("ba", "ea")),
    )
    return jax.shard_map(
        per_device,
        mesh=mesh,
        in_specs=placed,
        out_specs=(P("ea", None), P("ea"), P(), P(), P()),
        check_vma=False,
    )
```
